256 devices in a mesh: dp: 256 (over z, y, x, core).
Axes of the slice: x: 4, y: 4, z: 8, core: 2. Of those that a mesh axis runs over, the one named last changes fastest.
Arguments:
- tokens: bfloat16 [262144, 1024], P('dp'), may hold values from -80 to 80
- seg_ids: int32 [256, 1024], P('dp'), may hold values from 0 to 3, as said below
- counts: int32 [256], replicated, may hold values from 1 to 4, as said below
- positives: int32 [1024], P('dp'), may hold values from 0 to 1023, as said below
- w_qkv: bfloat16 [1024, 1536], replicated, may hold values from -0.1875 to 0.1875
- w_out: bfloat16 [512, 1024], replicated, may hold values from -0.25 to 0.25
- ln_gain: float32 [1024], replicated, may hold values from 0.1 to 1.9
- w_proj: bfloat16 [1024, 2048], replicated, may hold values from -0.1875 to 0.1875
Outputs:
- loss: float32 [1024], P('dp')
- grad_pooled: float32 [1024, 1024], P('dp')
The draws below stay inside these ranges and needn't reach their ends.
Inputs may be any that keep to these rules, and one draw needn't show every extreme that they name: `seg_ids`: within a rank, the ids never fall and every id from 0 to 3 occurs. Rank r's live segments are its slots 0 to counts[r] - 1; the other slots hold padding; some rank has all 4 live. `positives`: a live slot of another rank, as rank times 4 plus slot.
All inputs are finite; a program needn't handle non-finite values.
Results may differ from the reference program's by a relative error of at most 0.008.
Values may be sent and summed in bfloat16 or wider, within the bound.
No kernel may reach another device: no remote copies, remote signals or barrier semaphores. Data moves between devices by JAX's collectives and lax.ppermute only.
A program may use at most 192 MiB of HBM per device.

```python
import jax
import jax.numpy as jnp
from jax import lax

D = 1024
HEADS = 8
HEAD_DIM = 64
EMBED = 2048
TOK_DEV = 1024
SEG_DEV = 4
TOKENS = 262144
NKEYS = 1024
N_DP = 256


def segment_plan(key):
    key = jax.random.fold_in(key, 7)
    key_count, key_full, key_rank, key_pick, key_length = jax.random.split(key, 5)
    counts = jax.random.randint(key_count, (N_DP,), 1, SEG_DEV + 1, dtype=jnp.int32)
    full_rank = jax.random.randint(key_full, (), 0, N_DP, dtype=jnp.int32)
    counts = jnp.where(jnp.arange(N_DP, dtype=jnp.int32) == full_rank, SEG_DEV, counts).astype(jnp.int32)
    owner = jnp.repeat(jnp.arange(N_DP, dtype=jnp.int32), SEG_DEV)
    offset = jax.random.randint(key_rank, (NKEYS,), 1, N_DP, dtype=jnp.int32)
    target_rank = (owner + offset) % N_DP
    picks = jax.random.randint(key_pick, (NKEYS,), 0, 1048576, dtype=jnp.int32)
    target_slot = picks % counts[target_rank]
    positives = (target_rank * SEG_DEV + target_slot).astype(jnp.int32)
    length_weights = jax.random.randint(key_length, (N_DP, SEG_DEV), 1, 3, dtype=jnp.int32)
    cumulative = jnp.cumsum(length_weights, axis=1).astype(jnp.int32)
    total = cumulative[:, -1:]
    ends = (TOK_DEV - SEG_DEV) * cumulative // total
    starts = ends[:, :-1] + jnp.arange(1, SEG_DEV, dtype=jnp.int32)[None, :]
    position = jnp.arange(TOK_DEV, dtype=jnp.int32)
    segment = jnp.sum((position[None, :, None] >= starts[:, None, :]).astype(jnp.int32), axis=2)
    return (counts, positives, segment.astype(jnp.int32))


def draw_tokens(key, part):
    counts, positives, segment = segment_plan(key)
    key_base = jax.random.fold_in(key, 0)
    key_basis = jax.random.fold_in(key, 3)
    values = jnp.clip(jax.random.normal(key_base, (TOKENS, D), jnp.float32), -6.0, 6.0)
    basis = jnp.clip(jax.random.normal(key_basis, (NKEYS, D), jnp.float32), -4.0, 4.0)
    direction = basis + jnp.take(basis, positives, axis=0)
    slot_of = (jnp.arange(N_DP, dtype=jnp.int32)[:, None] * SEG_DEV + segment).reshape(TOKENS)
    values = values + jnp.take(direction, slot_of, axis=0)
    values = jnp.clip(values, -80.0, 80.0)
    return values.astype(jnp.bfloat16)


def draw_seg_ids(key, part):
    return segment_plan(key)[2]


def draw_counts(key, part):
    return segment_plan(key)[0]


def draw_positives(key, part):
    return segment_plan(key)[1]


def gaussian(own_key, shape, spread, limit, kind=jnp.bfloat16):
    drawn = jax.random.normal(own_key, shape, jnp.float32) * spread
    return jnp.minimum(jnp.maximum(drawn, -limit), limit).astype(kind)


def setup_inputs(seed: int = 0) -> dict:
    key_list = jax.random.split(jax.random.key(seed), 9)
    return {
        "tokens": draw_tokens(jax.random.fold_in(key_list[8], 71), 0),
        "seg_ids": draw_seg_ids(jax.random.fold_in(key_list[8], 71), 0),
        "counts": draw_counts(jax.random.fold_in(key_list[8], 71), 0),
        "positives": draw_positives(jax.random.fold_in(key_list[8], 71), 0),
        "w_qkv": gaussian(key_list[4], (D, 3 * HEADS * HEAD_DIM), D ** -0.5, 0.1875),
        "w_out": gaussian(key_list[5], (HEADS * HEAD_DIM, D), (HEADS * HEAD_DIM) ** -0.5, 0.25),
        "ln_gain": jnp.clip(1.0 + 0.18 * jax.random.normal(key_list[6], (D,), jnp.float32), 0.1, 1.9),
        "w_proj": gaussian(key_list[7], (D, EMBED), D ** -0.5, 0.1875),
    }


logit_scale = 20.0

def attend(tok_rows, segment, w_qkv, w_out, ln_gain):
    rows = tok_rows.shape[0]
    width = w_out.shape[0]
    head_dim = width // HEADS
    qkv = jnp.dot(tok_rows, w_qkv, preferred_element_type=jnp.float32).astype(jnp.bfloat16)
    qkv = qkv.reshape(rows, 3, HEADS, head_dim).astype(jnp.float32)
    scores = jnp.einsum('qhd,khd->hqk', qkv[:, 0], qkv[:, 1]) * head_dim ** (-0.5)
    same = segment[:, None] == segment[None, :]
    scores = jnp.where(same[None], scores, -1e+30)
    row_max = lax.optimization_barrier(jnp.max(scores, axis=-1, keepdims=True))
    exp_scores = jnp.exp(scores - row_max)
    probs = (exp_scores / lax.optimization_barrier(jnp.sum(exp_scores, axis=-1, keepdims=True))).astype(jnp.bfloat16)
    context = jnp.einsum('hqk,khd->qhd', probs.astype(jnp.float32), qkv[:, 2])
    context = context.astype(jnp.bfloat16).reshape(rows, width)
    resid = tok_rows.astype(jnp.float32) + jnp.dot(context, w_out, preferred_element_type=jnp.float32)
    centre = resid - lax.optimization_barrier(jnp.mean(resid, axis=-1, keepdims=True))
    variance = lax.optimization_barrier(jnp.mean(centre * centre, axis=-1, keepdims=True))
    return (centre * lax.rsqrt(variance + 1e-05) * ln_gain).astype(jnp.bfloat16)

def pool_rows(hidden, segment, slots):
    member = jnp.arange(slots, dtype=jnp.int32)[:, None] == segment[None, :]
    sums = jnp.dot(member.astype(jnp.bfloat16), hidden, preferred_element_type=jnp.float32)
    sizes = lax.optimization_barrier(jnp.sum(member.astype(jnp.float32), axis=1, keepdims=True))
    return (sums / sizes).astype(jnp.bfloat16)

def embed_rows(pooled, w_proj):
    proj = jnp.dot(pooled, w_proj, preferred_element_type=jnp.float32)
    rnorm = lax.rsqrt(lax.optimization_barrier(jnp.sum(proj * proj, axis=-1, keepdims=True)) + 1e-06)
    return (proj * rnorm, rnorm)

def reference(tokens, seg_ids, counts, positives, w_qkv, w_out, ln_gain, w_proj):
    ranks = tokens.reshape(N_DP, TOK_DEV, D)

    def one_rank(pair):
        hidden = attend(pair[0], pair[1], w_qkv, w_out, ln_gain)
        return pool_rows(hidden, pair[1], SEG_DEV)
    pooled = lax.map(one_rank, (ranks, seg_ids)).reshape(NKEYS, D)
    unit, rnorm = embed_rows(pooled, w_proj)
    emb = unit.astype(jnp.bfloat16)
    logits = logit_scale * jnp.dot(emb, emb.T, preferred_element_type=jnp.float32)
    slot_ids = jnp.arange(NKEYS, dtype=jnp.int32)
    live = slot_ids % SEG_DEV < jnp.repeat(counts, SEG_DEV).astype(jnp.int32)
    allowed = live[None, :] & (slot_ids[None, :] != slot_ids[:, None])
    exp_logits = jnp.where(allowed, jnp.exp(logits), 0.0)
    denominator = lax.optimization_barrier(jnp.sum(exp_logits, axis=-1))
    target = slot_ids[None, :] == positives[:, None]
    picked = lax.optimization_barrier(jnp.sum(jnp.where(target, logits, 0.0), axis=-1))
    loss = jnp.where(live, jnp.log(denominator) - picked, 0.0)
    weights = jnp.where(live[:, None], exp_logits / denominator[:, None] - target.astype(jnp.float32), 0.0)
    weights = weights.astype(jnp.bfloat16)
    d_emb = logit_scale * (jnp.dot(weights, emb, preferred_element_type=jnp.float32) + jnp.dot(weights.T, emb, preferred_element_type=jnp.float32))
    radial = lax.optimization_barrier(jnp.sum(d_emb * unit, axis=-1, keepdims=True))
    d_proj = ((d_emb - radial * unit) * rnorm).astype(jnp.bfloat16)
    grad_pooled = jnp.dot(d_proj, w_proj.T, preferred_element_type=jnp.float32)
    return (loss, grad_pooled)
```

```python
import functools
import math

import jax
import jax.numpy as jnp
from jax import lax
from jax.experimental import pallas as pl
from jax.experimental.pallas import tpu as pltpu
from jax.sharding import Mesh
from jax.sharding import PartitionSpec as P

AXES = ("dp_0", "dp_1", "dp_2", "dp_3")
HEADS = 8
HEAD_DIM = 64
PAIRS = HEADS // 2
LOG2E = math.log2(math.e)
LOGIT_SCALE = 20.0
META = 128
FAR = -1e30
BF16 = jnp.bfloat16
F32 = jnp.float32
VMEM_LIMIT = 60 * 1024 * 1024


def dot(a, b):
    return lax.dot_general(a, b, (((1,), (0,)), ((), ())), preferred_element_type=F32)


def dot_nt(a, b):
    return lax.dot_general(a, b, (((1,), (1,)), ((), ())), preferred_element_type=F32)


def rank_of():
    z, y, x, core = (lax.axis_index(a) for a in AXES)
    return ((z * 4 + y) * 4 + x) * 2 + core


def pool_kernel(
    seg_ref,
    counts_ref,
    positives_ref,
    x_hbm,
    wqkv_hbm,
    wout_hbm,
    gain_ref,
    out_ref,
    x_ref,
    wqkv_ref,
    wout_ref,
    q_ref,
    k_ref,
    v_ref,
    ctx_ref,
    sums_ref,
    sems,
    *,
    copies,
    tile,
):
    rows, width = x_ref.shape
    slots = out_ref.shape[1]
    hidden = HEADS * HEAD_DIM
    chunk = 256
    chunks = 3 * hidden // chunk

    x_copy = pltpu.make_async_copy(x_hbm, x_ref, sems.at[0])
    x_copy.start()
    w_copies = []
    for c in range(chunks):
        cols = slice(c * chunk, (c + 1) * chunk)
        w_copies.append(
            pltpu.make_async_copy(wqkv_hbm.at[:, cols], wqkv_ref.at[:, cols], sems.at[1 + c])
        )
        w_copies[-1].start()
    wout_copy = pltpu.make_async_copy(wout_hbm, wout_ref, sems.at[1 + chunks])
    wout_copy.start()

    seg = seg_ref[...]
    begins = [jnp.int32(0)]
    for s in range(1, slots):
        begins.append(jnp.sum((seg < s).astype(F32)).astype(jnp.int32))
    begins.append(jnp.int32(rows))

    row_id = lax.broadcasted_iota(jnp.int32, (rows, 2 * HEAD_DIM), 0)
    lane = lax.broadcasted_iota(jnp.int32, (rows, 2 * HEAD_DIM), 1)
    of_row = jnp.zeros((rows, 2 * HEAD_DIM), jnp.int32)
    for s in range(1, slots):
        of_row += (row_id >= begins[s]).astype(jnp.int32)
    feature = lane % HEAD_DIM
    mine = feature == of_row
    q_mark = jnp.where(mine, 1.0, 0.0).astype(BF16)
    k_mark = jnp.where(mine | (feature >= slots), 0.0, FAR).astype(BF16)
    first_half = lane < HEAD_DIM

    x_copy.wait()
    for c in range(chunks):
        w_copies[c].wait()
        kind, place = divmod(c * chunk, hidden)
        part = dot(x_ref[...], wqkv_ref[:, c * chunk : (c + 1) * chunk])
        if kind == 0:
            part = part * (LOG2E * HEAD_DIM**-0.5)
        part = part.astype(BF16)
        for p in range(chunk // (2 * HEAD_DIM)):
            pair = part[:, p * 2 * HEAD_DIM : (p + 1) * 2 * HEAD_DIM]
            head = place // HEAD_DIM + 2 * p
            if kind == 0:
                q_ref[head] = jnp.where(first_half, pair, q_mark)
                q_ref[head + 1] = jnp.where(first_half, q_mark, pair)
            elif kind == 1:
                k_ref[head] = jnp.where(first_half, pair, k_mark)
                k_ref[head + 1] = jnp.where(first_half, k_mark, pair)
            else:
                one = jnp.ones_like(pair)
                v_ref[head] = jnp.where(first_half, pair, one)
                v_ref[head + 1] = jnp.where(first_half, one, pair)

    wout_copy.wait()
    sums_ref[...] = jnp.zeros_like(sums_ref)
    half = lax.broadcasted_iota(jnp.int32, (tile, 2 * HEAD_DIM), 1) < HEAD_DIM
    key_tile = 128
    key_tiles = rows // key_tile
    widths = [w for w in (3, 4, 5, 6, 8) if w <= key_tiles]

    def one_tile(t, carry):
        r0 = pl.multiple_of(t * tile, tile)
        low = jnp.int32(0)
        high = jnp.int32(rows)
        for s in range(1, slots):
            low = jnp.where(begins[s] <= r0, begins[s], low)
        for s in range(slots - 1, 0, -1):
            high = jnp.where(begins[s] >= r0 + tile, begins[s], high)
        k0 = low // key_tile
        need = (high + key_tile - 1) // key_tile - k0

        for i, w in enumerate(widths):
            above = widths[i - 1] if i else 0

            @pl.when((need > above) & (need <= w))
            def _():
                start = pl.multiple_of(jnp.minimum(k0, key_tiles - w) * key_tile, key_tile)
                for p in range(PAIRS):
                    outs = []
                    for h in (2 * p, 2 * p + 1):
                        q = q_ref[h, pl.ds(r0, tile), :]
                        k = k_ref[h, pl.ds(start, w * key_tile), :]
                        v = v_ref[h, pl.ds(start, w * key_tile), :]
                        s = dot_nt(q, k)
                        e = jnp.exp2(s - jnp.max(s, axis=1, keepdims=True)).astype(BF16)
                        outs.append(dot(e, v))
                    top = jnp.where(half, outs[0], outs[1])
                    bottom = jnp.where(half, outs[1], outs[0])
                    bottom = pltpu.roll(bottom, HEAD_DIM, 1)
                    ctx_ref[:, p * 2 * HEAD_DIM : (p + 1) * 2 * HEAD_DIM] = (top / bottom).astype(BF16)

        resid = x_ref[pl.ds(r0, tile), :].astype(F32) + dot(ctx_ref[...], wout_ref[...])
        centre = resid - jnp.mean(resid, axis=1, keepdims=True)
        variance = jnp.mean(centre * centre, axis=1, keepdims=True)
        out = (centre * lax.rsqrt(variance + 1e-05) * gain_ref[...]).astype(BF16)
        slot = lax.broadcasted_iota(jnp.int32, (16, tile), 0)
        token = lax.broadcasted_iota(jnp.int32, (16, tile), 1) + r0
        member = jnp.zeros((16, tile), jnp.bool_)
        for s in range(slots):
            member |= (slot == s) & (token >= begins[s]) & (token < begins[s + 1])
        sums_ref[...] += dot(jnp.where(member, 1.0, 0.0).astype(BF16), out)
        return carry

    lax.fori_loop(0, rows // tile, one_tile, 0)

    slot_col = lax.broadcasted_iota(jnp.int32, (slots, 1), 0)
    sizes = jnp.ones((slots, 1), F32)
    for s in range(slots):
        sizes = jnp.where(slot_col == s, (begins[s + 1] - begins[s]).astype(F32), sizes)
    pooled = (sums_ref[0:slots, :] / sizes).astype(BF16)

    rank = rank_of()
    count = counts_ref[rank]
    line = lax.broadcasted_iota(jnp.int32, (slots, META), 0)
    col = lax.broadcasted_iota(jnp.int32, (slots, META), 1)
    positive = jnp.zeros((slots, META), jnp.int32)
    for s in range(slots):
        positive = jnp.where(line == s, positives_ref[s], positive)
    own = rank * slots + line
    meta = jnp.where(col == 0, positive >> 5, 0)
    meta = jnp.where(col == 1, positive & 31, meta)
    meta = jnp.where(col == 2, (line < count).astype(jnp.int32), meta)
    meta = jnp.where(col == 3, own >> 5, meta)
    meta = jnp.where(col == 4, own & 31, meta)
    meta = meta.astype(F32).astype(BF16)
    for i in range(copies):
        out_ref[i, :, 0:width] = pooled
        out_ref[i, :, width:] = meta


def pooled_rows(tokens, seg_ids, counts, positives, w_qkv, w_out, ln_gain, copies):
    rows, width = tokens.shape
    slots = positives.shape[0]
    hidden = w_out.shape[0]
    tile = 256
    any_spec = pl.BlockSpec(memory_space=pl.ANY)
    vmem = pl.BlockSpec(memory_space=pltpu.VMEM)
    smem = pl.BlockSpec(memory_space=pltpu.SMEM)
    return pl.pallas_call(
        functools.partial(pool_kernel, copies=copies, tile=tile),
        out_shape=jax.ShapeDtypeStruct((copies, slots, width + META), BF16),
        in_specs=[vmem, smem, smem, any_spec, any_spec, any_spec, vmem],
        out_specs=vmem,
        scratch_shapes=[
            pltpu.VMEM((rows, width), BF16),
            pltpu.VMEM((width, 3 * hidden), BF16),
            pltpu.VMEM((hidden, width), BF16),
            pltpu.VMEM((HEADS, rows, 2 * HEAD_DIM), BF16),
            pltpu.VMEM((HEADS, rows, 2 * HEAD_DIM), BF16),
            pltpu.VMEM((HEADS, rows, 2 * HEAD_DIM), BF16),
            pltpu.VMEM((tile, hidden), BF16),
            pltpu.VMEM((16, width), F32),
            pltpu.SemaphoreType.DMA((8,)),
        ],
        compiler_params=pltpu.CompilerParams(vmem_limit_bytes=VMEM_LIMIT),
        cost_estimate=pl.CostEstimate(
            flops=2 * rows * width * 4 * hidden + 4 * rows * rows * hidden,
            bytes_accessed=2 * (rows * width + 4 * width * hidden),
            transcendentals=HEADS * rows * rows // 2,
        ),
        name="pool",
    )(seg_ids, counts, positives, tokens, w_qkv, w_out, ln_gain.reshape(1, width))


def loss_kernel(
    mine_ref,
    other_ref,
    gram_ref,
    loss_ref,
    grad_ref,
    left_ref,
    right_ref,
    logit_ref,
    norm_ref,
):
    total, width = left_ref.shape
    part = total // 2
    slots = grad_ref.shape[0]
    block = 256
    gram = gram_ref[...]

    for b in range(total // block):
        ref = mine_ref if b * block < part else other_ref
        begin = b * block % part
        rows = slice(b * block, (b + 1) * block)
        pooled = ref[begin : begin + block, 0:width]
        through = dot(pooled, gram)
        wide = pooled.astype(F32)
        square = jnp.sum(through * wide, axis=1, keepdims=True)
        rnorm = lax.rsqrt(jnp.maximum(square, 0.0) + 1e-06)
        left_ref[rows, :] = (through * (rnorm * (LOGIT_SCALE * LOG2E))).astype(BF16)
        right_ref[rows, :] = (wide * rnorm).astype(BF16)
        norm_ref[rows, :] = jnp.broadcast_to(rnorm, (block, 128))

    meta = jnp.concatenate([mine_ref[:, width:], other_ref[:, width:]], axis=0)
    pick = lax.broadcasted_iota(jnp.int32, (16, META), 0) == lax.broadcasted_iota(
        jnp.int32, (16, META), 1
    )
    lines = dot_nt(pick.astype(F32).astype(BF16), meta)
    spread = (lax.broadcasted_iota(jnp.int32, (META, 128), 0) == 2).astype(F32).astype(BF16)
    live_col = dot(meta, spread)

    right = right_ref[...]
    sums = jnp.zeros((8, total), F32)
    for b in range(total // block):
        rows = slice(b * block, (b + 1) * block)
        logit = dot_nt(left_ref[rows, :], right)
        logit_ref[rows, :] = logit
        live = live_col[rows, :]
        pieces = []
        for c in range(total // 128):
            term = jnp.exp2(logit[:, c * 128 : (c + 1) * 128]) * live
            if b * block <= c * 128 < (b + 1) * block:
                row = lax.broadcasted_iota(jnp.int32, (block, 128), 0) + b * block
                col = lax.broadcasted_iota(jnp.int32, (block, 128), 1) + c * 128
                term = jnp.where(row == col, 0.0, term)
            pieces.append(jnp.sum(term.reshape(block // 8, 8, 128), axis=0))
        sums = sums + jnp.concatenate(pieces, axis=1)
    denominator_line = jnp.sum(sums, axis=0, keepdims=True)

    z, y, x, _ = (lax.axis_index(a) for a in AXES)
    begin = ((y * 4 + x) * 8 + z) * slots
    base = pl.multiple_of(begin // 16 * 16, 16)
    within = begin - base
    own_meta = mine_ref[pl.ds(base, 16), width:].astype(F32)
    own_positive = own_meta[:, 0:1] * 32.0 + own_meta[:, 1:2]
    own_live = own_meta[:, 2:3] > 0.5
    own_slot = own_meta[:, 3:4] * 32.0 + own_meta[:, 4:5]
    positive_line = lines[0:1, :] * 32.0 + lines[1:2, :]
    live_line = lines[2:3, :] > 0.5
    slot_line = lines[3:4, :] * 32.0 + lines[4:5, :]

    logit = logit_ref[pl.ds(base, 16), :]
    same = slot_line == own_slot
    raw = jnp.where(same, 0.0, jnp.exp2(logit))
    as_query = jnp.where(live_line, raw, 0.0)
    denominator = jnp.sum(as_query, axis=1, keepdims=True)
    target = slot_line == own_positive
    picked = jnp.sum(jnp.where(target, logit, 0.0), axis=1, keepdims=True) * (1.0 / LOG2E)
    loss = jnp.where(own_live, jnp.log(denominator) - picked, 0.0)
    for s in range(slots):
        row = lax.broadcasted_iota(jnp.int32, (16, 1), 0)
        loss_ref[s] = jnp.sum(jnp.where(row == within + s, loss, 0.0))
    query_weights = jnp.where(own_live, as_query / denominator - target.astype(F32), 0.0)
    hits = (positive_line == own_slot).astype(F32)
    key_weights = jnp.where(
        live_line, jnp.where(own_live, raw, 0.0) / denominator_line - hits, 0.0
    )
    weights = (query_weights + key_weights).astype(BF16)
    mix = dot(weights, right)
    image = dot(mix.astype(BF16), gram) * LOGIT_SCALE
    unit_image = left_ref[pl.ds(base, 16), :].astype(F32) * (1.0 / (LOGIT_SCALE * LOG2E))
    radial = LOGIT_SCALE * jnp.sum(mix * unit_image, axis=1, keepdims=True)
    rnorm = norm_ref[pl.ds(base, 16), 0:1]
    grad = (image - radial * unit_image) * rnorm
    out = grad[0:slots]
    for i in range(1, 16 // slots):
        out = jnp.where(within == i * slots, grad[i * slots : (i + 1) * slots], out)
    grad_ref[...] = out


def loss_and_grad(mine, other, gram, slots):
    part, padded = mine.shape
    width = padded - META
    total = 2 * part
    vmem = pl.BlockSpec(memory_space=pltpu.VMEM)
    return pl.pallas_call(
        loss_kernel,
        out_shape=(
            jax.ShapeDtypeStruct((slots,), F32),
            jax.ShapeDtypeStruct((slots, width), F32),
        ),
        in_specs=[vmem, vmem, vmem],
        out_specs=(pl.BlockSpec(memory_space=pltpu.SMEM), vmem),
        scratch_shapes=[
            pltpu.VMEM((total, width), BF16),
            pltpu.VMEM((total, width), BF16),
            pltpu.VMEM((total, total), F32),
            pltpu.VMEM((total, 128), F32),
        ],
        compiler_params=pltpu.CompilerParams(vmem_limit_bytes=VMEM_LIMIT),
        cost_estimate=pl.CostEstimate(
            flops=4 * total * total * width,
            bytes_accessed=4 * total * width,
            transcendentals=total * total,
        ),
        name="loss",
    )(mine, other, gram)


def body(tokens, seg_ids, counts, positives, w_qkv, w_out, ln_gain, w_proj):
    slots = positives.shape[0]
    z_size = lax.axis_size("dp_0")
    plane = ("dp_1", "dp_2")
    plane_size = lax.axis_size(plane)
    packed = pooled_rows(tokens, seg_ids, counts, positives, w_qkv, w_out, ln_gain, z_size)
    padded = packed.shape[-1]
    line = lax.all_to_all(packed, "dp_0", split_axis=0, concat_axis=0, tiled=True)
    line = line.reshape(z_size * slots, padded)
    copies = jnp.broadcast_to(line, (plane_size, *line.shape))
    mine = lax.all_to_all(copies, plane, split_axis=0, concat_axis=0, tiled=True)
    mine = mine.reshape(plane_size * z_size * slots, padded)
    other = lax.ppermute(mine, "dp_3", [(0, 1), (1, 0)])
    gram = lax.dot_general(
        w_proj, w_proj, (((1,), (1,)), ((), ())), preferred_element_type=F32
    ).astype(BF16)
    return loss_and_grad(mine, other, gram, slots)


def solution(mesh):
    finer = Mesh(mesh.devices.reshape(8, 4, 4, 2), AXES)
    return jax.shard_map(
        body,
        mesh=finer,
        in_specs=(P(AXES, None), P(AXES, None), P(), P(AXES), P(), P(), P(), P()),
        out_specs=(P(AXES), P(AXES, None)),
        check_vma=False,
    )
```

```python
import functools
import math

import jax
import jax.numpy as jnp
from jax import lax
from jax.experimental import pallas as pl
from jax.experimental.pallas import tpu as pltpu
from jax.sharding import Mesh
from jax.sharding import PartitionSpec as P

AXES = ("dp_0", "dp_1", "dp_2", "dp_3")
HEADS = 8
HEAD_DIM = 64
PAIRS = HEADS // 2
LOG2E = math.log2(math.e)
LOGIT_SCALE = 20.0
META = 128
FAR = -1e30
BF16 = jnp.bfloat16
F32 = jnp.float32
POOL_VMEM = 60 * 1024 * 1024
LOSS_VMEM = 24 * 1024 * 1024


def dot(a, b):
    return lax.dot_general(a, b, (((1,), (0,)), ((), ())), preferred_element_type=F32)


def dot_nt(a, b):
    return lax.dot_general(a, b, (((1,), (1,)), ((), ())), preferred_element_type=F32)


def rank_of():
    z, y, x, core = (lax.axis_index(a) for a in AXES)
    return ((z * 4 + y) * 4 + x) * 2 + core


def pool_kernel(
    seg_ref,
    counts_ref,
    positives_ref,
    x_hbm,
    wqkv_hbm,
    wout_hbm,
    gain_ref,
    out_ref,
    x_ref,
    wqkv_ref,
    wout_ref,
    q_ref,
    k_ref,
    v_ref,
    ctx_ref,
    sums_ref,
    sems,
    *,
    copies,
    tile,
):
    rows, width = x_ref.shape
    slots = out_ref.shape[1]
    hidden = HEADS * HEAD_DIM
    chunk = 256
    chunks = 3 * hidden // chunk

    x_copy = pltpu.make_async_copy(x_hbm, x_ref, sems.at[0])
    x_copy.start()
    w_copies = []
    for c in range(chunks):
        cols = slice(c * chunk, (c + 1) * chunk)
        w_copies.append(
            pltpu.make_async_copy(wqkv_hbm.at[:, cols], wqkv_ref.at[:, cols], sems.at[1 + c])
        )
        w_copies[-1].start()
    wout_copy = pltpu.make_async_copy(wout_hbm, wout_ref, sems.at[1 + chunks])
    wout_copy.start()

    seg = seg_ref[...]
    begins = [jnp.int32(0)]
    for s in range(1, slots):
        begins.append(jnp.sum((seg < s).astype(F32)).astype(jnp.int32))
    begins.append(jnp.int32(rows))

    row_id = lax.broadcasted_iota(jnp.int32, (rows, 2 * HEAD_DIM), 0)
    lane = lax.broadcasted_iota(jnp.int32, (rows, 2 * HEAD_DIM), 1)
    of_row = jnp.zeros((rows, 2 * HEAD_DIM), jnp.int32)
    for s in range(1, slots):
        of_row += (row_id >= begins[s]).astype(jnp.int32)
    feature = lane % HEAD_DIM
    mine = feature == of_row
    q_mark = jnp.where(mine, 1.0, 0.0).astype(BF16)
    k_mark = jnp.where(mine | (feature >= slots), 0.0, FAR).astype(BF16)
    first_half = lane < HEAD_DIM

    x_copy.wait()
    for c in range(chunks):
        w_copies[c].wait()
        kind, place = divmod(c * chunk, hidden)
        part = dot(x_ref[...], wqkv_ref[:, c * chunk : (c + 1) * chunk])
        if kind == 0:
            part = part * (LOG2E * HEAD_DIM**-0.5)
        part = part.astype(BF16)
        for p in range(chunk // (2 * HEAD_DIM)):
            pair = part[:, p * 2 * HEAD_DIM : (p + 1) * 2 * HEAD_DIM]
            head = place // HEAD_DIM + 2 * p
            if kind == 0:
                q_ref[head] = jnp.where(first_half, pair, q_mark)
                q_ref[head + 1] = jnp.where(first_half, q_mark, pair)
            elif kind == 1:
                k_ref[head] = jnp.where(first_half, pair, k_mark)
                k_ref[head + 1] = jnp.where(first_half, k_mark, pair)
            else:
                one = jnp.ones_like(pair)
                v_ref[head] = jnp.where(first_half, pair, one)
                v_ref[head + 1] = jnp.where(first_half, one, pair)

    wout_copy.wait()
    sums_ref[...] = jnp.zeros_like(sums_ref)
    half = lax.broadcasted_iota(jnp.int32, (tile, 2 * HEAD_DIM), 1) < HEAD_DIM
    key_tile = 128
    key_tiles = rows // key_tile
    widths = [w for w in (3, 4, 5, 6, 8) if w <= key_tiles]

    def one_tile(t, carry):
        r0 = pl.multiple_of(t * tile, tile)
        low = jnp.int32(0)
        high = jnp.int32(rows)
        for s in range(1, slots):
            low = jnp.where(begins[s] <= r0, begins[s], low)
        for s in range(slots - 1, 0, -1):
            high = jnp.where(begins[s] >= r0 + tile, begins[s], high)
        k0 = low // key_tile
        need = (high + key_tile - 1) // key_tile - k0

        for i, w in enumerate(widths):
            above = widths[i - 1] if i else 0

            @pl.when((need > above) & (need <= w))
            def _():
                start = pl.multiple_of(jnp.minimum(k0, key_tiles - w) * key_tile, key_tile)
                for p in range(PAIRS):
                    outs = []
                    for h in (2 * p, 2 * p + 1):
                        q = q_ref[h, pl.ds(r0, tile), :]
                        k = k_ref[h, pl.ds(start, w * key_tile), :]
                        v = v_ref[h, pl.ds(start, w * key_tile), :]
                        s = dot_nt(q, k)
                        e = jnp.exp2(s - jnp.max(s, axis=1, keepdims=True)).astype(BF16)
                        outs.append(dot(e, v))
                    top = jnp.where(half, outs[0], outs[1])
                    bottom = jnp.where(half, outs[1], outs[0])
                    bottom = pltpu.roll(bottom, HEAD_DIM, 1)
                    ctx_ref[:, p * 2 * HEAD_DIM : (p + 1) * 2 * HEAD_DIM] = (top / bottom).astype(BF16)

        resid = x_ref[pl.ds(r0, tile), :].astype(F32) + dot(ctx_ref[...], wout_ref[...])
        centre = resid - jnp.mean(resid, axis=1, keepdims=True)
        variance = jnp.mean(centre * centre, axis=1, keepdims=True)
        out = (centre * lax.rsqrt(variance + 1e-05) * gain_ref[...]).astype(BF16)
        slot = lax.broadcasted_iota(jnp.int32, (16, tile), 0)
        token = lax.broadcasted_iota(jnp.int32, (16, tile), 1) + r0
        member = jnp.zeros((16, tile), jnp.bool_)
        for s in range(slots):
            member |= (slot == s) & (token >= begins[s]) & (token < begins[s + 1])
        sums_ref[...] += dot(jnp.where(member, 1.0, 0.0).astype(BF16), out)
        return carry

    lax.fori_loop(0, rows // tile, one_tile, 0)

    slot_col = lax.broadcasted_iota(jnp.int32, (slots, 1), 0)
    sizes = jnp.ones((slots, 1), F32)
    for s in range(slots):
        sizes = jnp.where(slot_col == s, (begins[s + 1] - begins[s]).astype(F32), sizes)
    pooled = (sums_ref[0:slots, :] / sizes).astype(BF16)

    rank = rank_of()
    count = counts_ref[rank]
    line = lax.broadcasted_iota(jnp.int32, (slots, META), 0)
    col = lax.broadcasted_iota(jnp.int32, (slots, META), 1)
    positive = jnp.zeros((slots, META), jnp.int32)
    for s in range(slots):
        positive = jnp.where(line == s, positives_ref[s], positive)
    own = rank * slots + line
    meta = jnp.where(col == 0, positive >> 5, 0)
    meta = jnp.where(col == 1, positive & 31, meta)
    meta = jnp.where(col == 2, (line < count).astype(jnp.int32), meta)
    meta = jnp.where(col == 3, own >> 5, meta)
    meta = jnp.where(col == 4, own & 31, meta)
    meta = meta.astype(F32).astype(BF16)
    for i in range(copies):
        out_ref[i, :, 0:width] = pooled
        out_ref[i, :, width:] = meta


def pooled_rows(tokens, seg_ids, counts, positives, w_qkv, w_out, ln_gain, copies):
    rows, width = tokens.shape
    slots = positives.shape[0]
    hidden = w_out.shape[0]
    tile = 256
    any_spec = pl.BlockSpec(memory_space=pltpu.HBM)
    vmem = pl.BlockSpec(memory_space=pltpu.VMEM)
    smem = pl.BlockSpec(memory_space=pltpu.SMEM)
    return pl.pallas_call(
        functools.partial(pool_kernel, copies=copies, tile=tile),
        out_shape=jax.ShapeDtypeStruct((copies, slots, width + META), BF16),
        in_specs=[vmem, smem, smem, any_spec, any_spec, any_spec, vmem],
        out_specs=vmem,
        scratch_shapes=[
            pltpu.VMEM((rows, width), BF16),
            pltpu.VMEM((width, 3 * hidden), BF16),
            pltpu.VMEM((hidden, width), BF16),
            pltpu.VMEM((HEADS, rows, 2 * HEAD_DIM), BF16),
            pltpu.VMEM((HEADS, rows, 2 * HEAD_DIM), BF16),
            pltpu.VMEM((HEADS, rows, 2 * HEAD_DIM), BF16),
            pltpu.VMEM((tile, hidden), BF16),
            pltpu.VMEM((16, width), F32),
            pltpu.SemaphoreType.DMA((8,)),
        ],
        compiler_params=pltpu.CompilerParams(vmem_limit_bytes=POOL_VMEM),
        cost_estimate=pl.CostEstimate(
            flops=2 * rows * width * 4 * hidden + 4 * rows * rows * hidden,
            bytes_accessed=2 * (rows * width + 4 * width * hidden),
            transcendentals=HEADS * rows * rows // 2,
        ),
        name="pool",
    )(seg_ids, counts, positives, tokens, w_qkv, w_out, ln_gain.reshape(1, width))


def loss_kernel(
    mine_ref,
    other_ref,
    gram_ref,
    loss_ref,
    grad_ref,
    left_ref,
    right_ref,
    logit_ref,
    norm_ref,
):
    total, width = left_ref.shape
    part = total // 2
    slots = grad_ref.shape[0]
    block = 256
    gram = gram_ref[...]

    for b in range(total // block):
        ref = mine_ref if b * block < part else other_ref
        begin = b * block % part
        rows = slice(b * block, (b + 1) * block)
        pooled = ref[begin : begin + block, 0:width]
        through = dot(pooled, gram)
        wide = pooled.astype(F32)
        square = jnp.sum(through * wide, axis=1, keepdims=True)
        rnorm = lax.rsqrt(jnp.maximum(square, 0.0) + 1e-06)
        left_ref[rows, :] = (through * (rnorm * (LOGIT_SCALE * LOG2E))).astype(BF16)
        right_ref[rows, :] = (wide * rnorm).astype(BF16)
        norm_ref[rows, :] = jnp.broadcast_to(rnorm, (block, 128))

    meta = jnp.concatenate([mine_ref[:, width:], other_ref[:, width:]], axis=0)
    pick = lax.broadcasted_iota(jnp.int32, (16, META), 0) == lax.broadcasted_iota(
        jnp.int32, (16, META), 1
    )
    lines = dot_nt(pick.astype(F32).astype(BF16), meta)
    spread = (lax.broadcasted_iota(jnp.int32, (META, 128), 0) == 2).astype(F32).astype(BF16)
    live_col = dot(meta, spread)

    right = right_ref[...]
    sums = jnp.zeros((8, total), F32)
    for b in range(total // block):
        rows = slice(b * block, (b + 1) * block)
        logit = dot_nt(left_ref[rows, :], right)
        logit_ref[rows, :] = logit
        live = live_col[rows, :]
        pieces = []
        for c in range(total // 128):
            term = jnp.exp2(logit[:, c * 128 : (c + 1) * 128]) * live
            if b * block <= c * 128 < (b + 1) * block:
                row = lax.broadcasted_iota(jnp.int32, (block, 128), 0) + b * block
                col = lax.broadcasted_iota(jnp.int32, (block, 128), 1) + c * 128
                term = jnp.where(row == col, 0.0, term)
            pieces.append(jnp.sum(term.reshape(block // 8, 8, 128), axis=0))
        sums = sums + jnp.concatenate(pieces, axis=1)
    denominator_line = jnp.sum(sums, axis=0, keepdims=True)

    z, y, x, _ = (lax.axis_index(a) for a in AXES)
    begin = ((y * 4 + x) * 8 + z) * slots
    base = pl.multiple_of(begin // 16 * 16, 16)
    within = begin - base
    own_meta = mine_ref[pl.ds(base, 16), width:].astype(F32)
    own_positive = own_meta[:, 0:1] * 32.0 + own_meta[:, 1:2]
    own_live = own_meta[:, 2:3] > 0.5
    own_slot = own_meta[:, 3:4] * 32.0 + own_meta[:, 4:5]
    positive_line = lines[0:1, :] * 32.0 + lines[1:2, :]
    live_line = lines[2:3, :] > 0.5
    slot_line = lines[3:4, :] * 32.0 + lines[4:5, :]

    logit = logit_ref[pl.ds(base, 16), :]
    same = slot_line == own_slot
    raw = jnp.where(same, 0.0, jnp.exp2(logit))
    as_query = jnp.where(live_line, raw, 0.0)
    denominator = jnp.sum(as_query, axis=1, keepdims=True)
    target = slot_line == own_positive
    picked = jnp.sum(jnp.where(target, logit, 0.0), axis=1, keepdims=True) * (1.0 / LOG2E)
    loss = jnp.where(own_live, jnp.log(denominator) - picked, 0.0)
    for s in range(slots):
        row = lax.broadcasted_iota(jnp.int32, (16, 1), 0)
        loss_ref[s] = jnp.sum(jnp.where(row == within + s, loss, 0.0))
    query_weights = jnp.where(own_live, as_query / denominator - target.astype(F32), 0.0)
    hits = (positive_line == own_slot).astype(F32)
    key_weights = jnp.where(
        live_line, jnp.where(own_live, raw, 0.0) / denominator_line - hits, 0.0
    )
    weights = (query_weights + key_weights).astype(BF16)
    mix = dot(weights, right)
    image = dot(mix.astype(BF16), gram) * LOGIT_SCALE
    unit_image = left_ref[pl.ds(base, 16), :].astype(F32) * (1.0 / (LOGIT_SCALE * LOG2E))
    radial = LOGIT_SCALE * jnp.sum(mix * unit_image, axis=1, keepdims=True)
    rnorm = norm_ref[pl.ds(base, 16), 0:1]
    grad = (image - radial * unit_image) * rnorm
    out = grad[0:slots]
    for i in range(1, 16 // slots):
        out = jnp.where(within == i * slots, grad[i * slots : (i + 1) * slots], out)
    grad_ref[...] = out


def loss_and_grad(mine, other, gram, slots):
    part, padded = mine.shape
    width = padded - META
    total = 2 * part
    vmem = pl.BlockSpec(memory_space=pltpu.VMEM)
    return pl.pallas_call(
        loss_kernel,
        out_shape=(
            jax.ShapeDtypeStruct((slots,), F32),
            jax.ShapeDtypeStruct((slots, width), F32),
        ),
        in_specs=[vmem, vmem, vmem],
        out_specs=(pl.BlockSpec(memory_space=pltpu.SMEM), vmem),
        scratch_shapes=[
            pltpu.VMEM((total, width), BF16),
            pltpu.VMEM((total, width), BF16),
            pltpu.VMEM((total, total), F32),
            pltpu.VMEM((total, 128), F32),
        ],
        compiler_params=pltpu.CompilerParams(vmem_limit_bytes=LOSS_VMEM),
        cost_estimate=pl.CostEstimate(
            flops=4 * total * total * width,
            bytes_accessed=4 * total * width,
            transcendentals=total * total,
        ),
        name="loss",
    )(mine, other, gram)


def body(tokens, seg_ids, counts, positives, w_qkv, w_out, ln_gain, w_proj):
    slots = positives.shape[0]
    z_size = lax.axis_size("dp_0")
    plane = ("dp_1", "dp_2")
    plane_size = lax.axis_size(plane)
    packed = pooled_rows(tokens, seg_ids, counts, positives, w_qkv, w_out, ln_gain, z_size)
    padded = packed.shape[-1]
    w_proj, packed = lax.optimization_barrier((w_proj, packed))
    gram = lax.dot_general(
        w_proj, w_proj, (((1,), (1,)), ((), ())), preferred_element_type=F32
    ).astype(BF16)
    line = lax.all_to_all(packed, "dp_0", split_axis=0, concat_axis=0, tiled=True)
    line = line.reshape(z_size * slots, padded)
    copies = jnp.broadcast_to(line, (plane_size, *line.shape))
    mine = lax.all_to_all(copies, plane, split_axis=0, concat_axis=0, tiled=True)
    mine = mine.reshape(plane_size * z_size * slots, padded)
    mine, gram = lax.optimization_barrier((mine, gram))
    other = lax.ppermute(mine, "dp_3", [(0, 1), (1, 0)])
    return loss_and_grad(mine, other, gram, slots)


def solution(mesh):
    finer = Mesh(mesh.devices.reshape(8, 4, 4, 2), AXES)
    return jax.shard_map(
        body,
        mesh=finer,
        in_specs=(P(AXES, None), P(AXES, None), P(), P(AXES), P(), P(), P(), P()),
        out_specs=(P(AXES), P(AXES, None)),
        check_vma=False,
    )
```

```python
import functools
import math

import jax
import jax.numpy as jnp
from jax import lax
from jax.experimental import pallas as pl
from jax.experimental.pallas import tpu as pltpu
from jax.sharding import Mesh
from jax.sharding import PartitionSpec as P

AXES = ("dp_0", "dp_1", "dp_2", "dp_3")
HEADS = 8
HEAD_DIM = 64
PAIRS = HEADS // 2
LOG2E = math.log2(math.e)
LOGIT_SCALE = 20.0
META = 128
ONES = 16
FAR = -1e30
BF16 = jnp.bfloat16
F32 = jnp.float32
POOL_VMEM = 60 * 1024 * 1024
LOSS_VMEM = 24 * 1024 * 1024


def dot(a, b):
    return lax.dot_general(a, b, (((1,), (0,)), ((), ())), preferred_element_type=F32)


def dot_nt(a, b):
    return lax.dot_general(a, b, (((1,), (1,)), ((), ())), preferred_element_type=F32)


def dot_tn(a, b):
    return lax.dot_general(a, b, (((0,), (0,)), ((), ())), preferred_element_type=F32)


def rank_of():
    z, y, x, core = (lax.axis_index(a) for a in AXES)
    return ((z * 4 + y) * 4 + x) * 2 + core


def pool_kernel(
    seg_ref,
    counts_ref,
    positives_ref,
    x_hbm,
    wqkv_hbm,
    wout_hbm,
    gain_ref,
    out_ref,
    x_ref,
    wqkv_ref,
    wout_ref,
    q_ref,
    k_ref,
    v_ref,
    ctx_ref,
    sums_ref,
    sems,
    *,
    copies,
    tile,
):
    rows, width = x_ref.shape
    slots = out_ref.shape[1]
    hidden = HEADS * HEAD_DIM
    chunk = 256
    chunks = 3 * hidden // chunk

    x_copy = pltpu.make_async_copy(x_hbm, x_ref, sems.at[0])
    x_copy.start()
    w_copies = []
    for c in range(chunks):
        cols = slice(c * chunk, (c + 1) * chunk)
        w_copies.append(
            pltpu.make_async_copy(wqkv_hbm.at[:, cols], wqkv_ref.at[:, cols], sems.at[1 + c])
        )
        w_copies[-1].start()
    wout_copy = pltpu.make_async_copy(wout_hbm, wout_ref, sems.at[1 + chunks])
    wout_copy.start()

    seg = seg_ref[...]
    begins = [jnp.int32(0)]
    for s in range(1, slots):
        begins.append(jnp.sum((seg < s).astype(F32)).astype(jnp.int32))
    begins.append(jnp.int32(rows))

    row_id = lax.broadcasted_iota(jnp.int32, (rows, 2 * HEAD_DIM), 0)
    lane = lax.broadcasted_iota(jnp.int32, (rows, 2 * HEAD_DIM), 1)
    of_row = jnp.zeros((rows, 2 * HEAD_DIM), jnp.int32)
    for s in range(1, slots):
        of_row += (row_id >= begins[s]).astype(jnp.int32)
    feature = lane % HEAD_DIM
    mine = feature == of_row
    q_mark = jnp.where(mine, 1.0, 0.0).astype(BF16)
    k_mark = jnp.where(mine | (feature >= slots), 0.0, FAR).astype(BF16)
    first_half = lane < HEAD_DIM

    x_copy.wait()
    def project(kind, g, carry):
        c0 = pl.multiple_of(kind * hidden + g * chunk, chunk)
        part = dot(x_ref[...], wqkv_ref[:, pl.ds(c0, chunk)])
        if kind == 0:
            part = part * (LOG2E * HEAD_DIM**-0.5)
        part = part.astype(BF16)
        for p in range(chunk // (2 * HEAD_DIM)):
            pair = part[:, p * 2 * HEAD_DIM : (p + 1) * 2 * HEAD_DIM]
            head = g * (chunk // HEAD_DIM) + 2 * p
            if kind == 0:
                q_ref[head] = jnp.where(first_half, pair, q_mark)
                q_ref[head + 1] = jnp.where(first_half, q_mark, pair)
            elif kind == 1:
                k_ref[head] = jnp.where(first_half, pair, k_mark)
                k_ref[head + 1] = jnp.where(first_half, k_mark, pair)
            else:
                turned = pair.T
                for i in range(2):
                    v_ref[head + i, 0:HEAD_DIM, :] = turned[i * HEAD_DIM : (i + 1) * HEAD_DIM]
                    v_ref[head + i, HEAD_DIM:, :] = jnp.ones((ONES, rows), BF16)
        return carry

    for kind in range(3):
        for c in range(kind * chunks // 3, (kind + 1) * chunks // 3):
            w_copies[c].wait()
        lax.fori_loop(0, chunks // 3, functools.partial(project, kind), 0)

    wout_copy.wait()
    sums_ref[...] = jnp.zeros_like(sums_ref)
    ctx_ref[...] = jnp.zeros_like(ctx_ref)
    key_tile = 128
    key_tiles = rows // key_tile
    widths = [w for w in (3, 4, 5, 6, 8) if w <= key_tiles]

    def project_out(r0):
        return x_ref[pl.ds(r0, tile), :].astype(F32) + dot_tn(ctx_ref[...], wout_ref[...])

    def pool_tile(resid, r0, valid):
        centre = resid - jnp.mean(resid, axis=1, keepdims=True)
        variance = jnp.mean(centre * centre, axis=1, keepdims=True)
        out = (centre * lax.rsqrt(variance + 1e-05) * gain_ref[...]).astype(BF16)
        slot = lax.broadcasted_iota(jnp.int32, (16, tile), 0)
        token = lax.broadcasted_iota(jnp.int32, (16, tile), 1) + r0
        member = jnp.zeros((16, tile), jnp.bool_)
        for s in range(slots):
            member |= (slot == s) & (token >= begins[s]) & (token < begins[s + 1])
        member = jnp.where(member & valid, 1.0, 0.0).astype(BF16)
        sums_ref[...] += dot(member, out)

    def one_tile(t, carry):
        r0 = pl.multiple_of(t * tile, tile)
        last = pl.multiple_of(jnp.maximum(r0 - tile, 0), tile)
        low = jnp.int32(0)
        high = jnp.int32(rows)
        for s in range(1, slots):
            low = jnp.where(begins[s] <= r0, begins[s], low)
        for s in range(slots - 1, 0, -1):
            high = jnp.where(begins[s] >= r0 + tile, begins[s], high)
        k0 = low // key_tile
        need = (high + key_tile - 1) // key_tile - k0

        for i, w in enumerate(widths):
            above = widths[i - 1] if i else 0

            @pl.when((need > above) & (need <= w))
            def _():
                start = pl.multiple_of(jnp.minimum(k0, key_tiles - w) * key_tile, key_tile)
                def score(h):
                    q = q_ref[h, pl.ds(r0, tile), :]
                    k = k_ref[h, pl.ds(start, w * key_tile), :]
                    return dot_nt(k, q)

                def soften(s):
                    return jnp.exp2(s - jnp.max(s, axis=0, keepdims=True)).astype(BF16)

                def finish(h, e):
                    v = v_ref[h, :, pl.ds(start, w * key_tile)]
                    out = dot(v, e)
                    part = out[0:HEAD_DIM] / out[HEAD_DIM : HEAD_DIM + 1]
                    ctx_ref[h * HEAD_DIM : (h + 1) * HEAD_DIM, :] = part.astype(BF16)

                resid = project_out(last)
                ahead = [score(0), score(1)]
                for h in range(0, HEADS, 2):
                    now = ahead
                    if h + 2 < HEADS:
                        ahead = [score(h + 2), score(h + 3)]
                    es = [soften(s) for s in now]
                    for i in range(2):
                        finish(h + i, es[i])
                    if h == 2:
                        pool_tile(resid, last, t > 0)

        return carry

    lax.fori_loop(0, rows // tile, one_tile, 0)
    last = rows - tile
    pool_tile(project_out(last), last, True)

    slot_col = lax.broadcasted_iota(jnp.int32, (slots, 1), 0)
    sizes = jnp.ones((slots, 1), F32)
    for s in range(slots):
        sizes = jnp.where(slot_col == s, (begins[s + 1] - begins[s]).astype(F32), sizes)
    pooled = (sums_ref[0:slots, :] / sizes).astype(BF16)

    rank = rank_of()
    count = counts_ref[rank]
    line = lax.broadcasted_iota(jnp.int32, (slots, META), 0)
    col = lax.broadcasted_iota(jnp.int32, (slots, META), 1)
    positive = jnp.zeros((slots, META), jnp.int32)
    for s in range(slots):
        positive = jnp.where(line == s, positives_ref[s], positive)
    own = rank * slots + line
    meta = jnp.where(col == 0, positive >> 5, 0)
    meta = jnp.where(col == 1, positive & 31, meta)
    meta = jnp.where(col == 2, (line < count).astype(jnp.int32), meta)
    meta = jnp.where(col == 3, own >> 5, meta)
    meta = jnp.where(col == 4, own & 31, meta)
    meta = meta.astype(F32).astype(BF16)
    for i in range(copies):
        out_ref[i, :, 0:width] = pooled
        out_ref[i, :, width:] = meta


def pooled_rows(tokens, seg_ids, counts, positives, w_qkv, w_out, ln_gain, copies):
    rows, width = tokens.shape
    slots = positives.shape[0]
    hidden = w_out.shape[0]
    tile = 256
    any_spec = pl.BlockSpec(memory_space=pltpu.HBM)
    vmem = pl.BlockSpec(memory_space=pltpu.VMEM)
    smem = pl.BlockSpec(memory_space=pltpu.SMEM)
    return pl.pallas_call(
        functools.partial(pool_kernel, copies=copies, tile=tile),
        out_shape=jax.ShapeDtypeStruct((copies, slots, width + META), BF16),
        in_specs=[vmem, smem, smem, any_spec, any_spec, any_spec, vmem],
        out_specs=vmem,
        scratch_shapes=[
            pltpu.VMEM((rows, width), BF16),
            pltpu.VMEM((width, 3 * hidden), BF16),
            pltpu.VMEM((hidden, width), BF16),
            pltpu.VMEM((HEADS, rows, 2 * HEAD_DIM), BF16),
            pltpu.VMEM((HEADS, rows, 2 * HEAD_DIM), BF16),
            pltpu.VMEM((HEADS, HEAD_DIM + ONES, rows), BF16),
            pltpu.VMEM((hidden, tile), BF16),
            pltpu.VMEM((16, width), F32),
            pltpu.SemaphoreType.DMA((8,)),
        ],
        compiler_params=pltpu.CompilerParams(vmem_limit_bytes=POOL_VMEM),
        cost_estimate=pl.CostEstimate(
            flops=2 * rows * width * 4 * hidden + 4 * rows * rows * hidden,
            bytes_accessed=2 * (rows * width + 4 * width * hidden),
            transcendentals=HEADS * rows * rows // 2,
        ),
        name="pool",
    )(seg_ids, counts, positives, tokens, w_qkv, w_out, ln_gain.reshape(1, width))


def loss_kernel(
    mine_ref,
    other_ref,
    gram_ref,
    loss_ref,
    grad_ref,
    left_ref,
    right_ref,
    logit_ref,
    norm_ref,
):
    total, width = left_ref.shape
    part = total // 2
    slots = grad_ref.shape[0]
    block = 256
    gram = gram_ref[...]

    for b in range(total // block):
        ref = mine_ref if b * block < part else other_ref
        begin = b * block % part
        rows = slice(b * block, (b + 1) * block)
        pooled = ref[begin : begin + block, 0:width]
        through = dot(pooled, gram)
        wide = pooled.astype(F32)
        square = jnp.sum(through * wide, axis=1, keepdims=True)
        rnorm = lax.rsqrt(jnp.maximum(square, 0.0) + 1e-06)
        left_ref[rows, :] = (through * (rnorm * (LOGIT_SCALE * LOG2E))).astype(BF16)
        right_ref[rows, :] = (wide * rnorm).astype(BF16)
        norm_ref[rows, :] = jnp.broadcast_to(rnorm, (block, 128))

    meta = jnp.concatenate([mine_ref[:, width:], other_ref[:, width:]], axis=0)
    pick = lax.broadcasted_iota(jnp.int32, (16, META), 0) == lax.broadcasted_iota(
        jnp.int32, (16, META), 1
    )
    lines = dot_nt(pick.astype(F32).astype(BF16), meta)
    spread = (lax.broadcasted_iota(jnp.int32, (META, 128), 0) == 2).astype(F32).astype(BF16)
    live_col = dot(meta, spread)

    right = right_ref[...]
    sums = jnp.zeros((8, total), F32)
    for b in range(total // block):
        rows = slice(b * block, (b + 1) * block)
        logit = dot_nt(left_ref[rows, :], right)
        logit_ref[rows, :] = logit
        live = live_col[rows, :]
        pieces = []
        for c in range(total // 128):
            term = jnp.exp2(logit[:, c * 128 : (c + 1) * 128]) * live
            if b * block <= c * 128 < (b + 1) * block:
                row = lax.broadcasted_iota(jnp.int32, (block, 128), 0) + b * block
                col = lax.broadcasted_iota(jnp.int32, (block, 128), 1) + c * 128
                term = jnp.where(row == col, 0.0, term)
            pieces.append(jnp.sum(term.reshape(block // 8, 8, 128), axis=0))
        sums = sums + jnp.concatenate(pieces, axis=1)
    denominator_line = jnp.sum(sums, axis=0, keepdims=True)

    z, y, x, _ = (lax.axis_index(a) for a in AXES)
    begin = ((y * 4 + x) * 8 + z) * slots
    base = pl.multiple_of(begin // 16 * 16, 16)
    within = begin - base
    own_meta = mine_ref[pl.ds(base, 16), width:].astype(F32)
    own_positive = own_meta[:, 0:1] * 32.0 + own_meta[:, 1:2]
    own_live = own_meta[:, 2:3] > 0.5
    own_slot = own_meta[:, 3:4] * 32.0 + own_meta[:, 4:5]
    positive_line = lines[0:1, :] * 32.0 + lines[1:2, :]
    live_line = lines[2:3, :] > 0.5
    slot_line = lines[3:4, :] * 32.0 + lines[4:5, :]

    logit = logit_ref[pl.ds(base, 16), :]
    same = slot_line == own_slot
    raw = jnp.where(same, 0.0, jnp.exp2(logit))
    as_query = jnp.where(live_line, raw, 0.0)
    denominator = jnp.sum(as_query, axis=1, keepdims=True)
    target = slot_line == own_positive
    picked = jnp.sum(jnp.where(target, logit, 0.0), axis=1, keepdims=True) * (1.0 / LOG2E)
    loss = jnp.where(own_live, jnp.log(denominator) - picked, 0.0)
    for s in range(slots):
        row = lax.broadcasted_iota(jnp.int32, (16, 1), 0)
        loss_ref[s] = jnp.sum(jnp.where(row == within + s, loss, 0.0))
    query_weights = jnp.where(own_live, as_query / denominator - target.astype(F32), 0.0)
    hits = (positive_line == own_slot).astype(F32)
    key_weights = jnp.where(
        live_line, jnp.where(own_live, raw, 0.0) / denominator_line - hits, 0.0
    )
    weights = (query_weights + key_weights).astype(BF16)
    mix = dot(weights, right)
    image = dot(mix.astype(BF16), gram) * LOGIT_SCALE
    unit_image = left_ref[pl.ds(base, 16), :].astype(F32) * (1.0 / (LOGIT_SCALE * LOG2E))
    radial = LOGIT_SCALE * jnp.sum(mix * unit_image, axis=1, keepdims=True)
    rnorm = norm_ref[pl.ds(base, 16), 0:1]
    grad = (image - radial * unit_image) * rnorm
    out = grad[0:slots]
    for i in range(1, 16 // slots):
        out = jnp.where(within == i * slots, grad[i * slots : (i + 1) * slots], out)
    grad_ref[...] = out


def loss_and_grad(mine, other, gram, slots):
    part, padded = mine.shape
    width = padded - META
    total = 2 * part
    vmem = pl.BlockSpec(memory_space=pltpu.VMEM)
    return pl.pallas_call(
        loss_kernel,
        out_shape=(
            jax.ShapeDtypeStruct((slots,), F32),
            jax.ShapeDtypeStruct((slots, width), F32),
        ),
        in_specs=[vmem, vmem, vmem],
        out_specs=(pl.BlockSpec(memory_space=pltpu.SMEM), vmem),
        scratch_shapes=[
            pltpu.VMEM((total, width), BF16),
            pltpu.VMEM((total, width), BF16),
            pltpu.VMEM((total, total), F32),
            pltpu.VMEM((total, 128), F32),
        ],
        compiler_params=pltpu.CompilerParams(vmem_limit_bytes=LOSS_VMEM),
        cost_estimate=pl.CostEstimate(
            flops=4 * total * total * width,
            bytes_accessed=4 * total * width,
            transcendentals=total * total,
        ),
        name="loss",
    )(mine, other, gram)


def body(tokens, seg_ids, counts, positives, w_qkv, w_out, ln_gain, w_proj):
    slots = positives.shape[0]
    z_size = lax.axis_size("dp_0")
    plane = ("dp_1", "dp_2")
    plane_size = lax.axis_size(plane)
    packed = pooled_rows(tokens, seg_ids, counts, positives, w_qkv, w_out, ln_gain, z_size)
    padded = packed.shape[-1]
    w_proj, packed = lax.optimization_barrier((w_proj, packed))
    gram = lax.dot_general(
        w_proj, w_proj, (((1,), (1,)), ((), ())), preferred_element_type=F32
    ).astype(BF16)
    line = lax.all_to_all(packed, "dp_0", split_axis=0, concat_axis=0, tiled=True)
    line = line.reshape(z_size * slots, padded)
    copies = jnp.broadcast_to(line, (plane_size, *line.shape))
    mine = lax.all_to_all(copies, plane, split_axis=0, concat_axis=0, tiled=True)
    mine = mine.reshape(plane_size * z_size * slots, padded)
    mine, gram = lax.optimization_barrier((mine, gram))
    other = lax.ppermute(mine, "dp_3", [(0, 1), (1, 0)])
    return loss_and_grad(mine, other, gram, slots)


def solution(mesh):
    finer = Mesh(mesh.devices.reshape(8, 4, 4, 2), AXES)
    return jax.shard_map(
        body,
        mesh=finer,
        in_specs=(P(AXES, None), P(AXES, None), P(), P(AXES), P(), P(), P(), P()),
        out_specs=(P(AXES), P(AXES, None)),
        check_vma=False,
    )
```

```python
import functools
import math

import jax
import jax.numpy as jnp
from jax import lax
from jax.experimental import pallas as pl
from jax.experimental.pallas import tpu as pltpu
from jax.sharding import Mesh
from jax.sharding import PartitionSpec as P

AXES = ("dp_0", "dp_1", "dp_2", "dp_3")
HEADS = 8
HEAD_DIM = 64
PAIRS = HEADS // 2
LOG2E = math.log2(math.e)
LOGIT_SCALE = 20.0
META = 128
ONES = 16
FAR = -1e30
BF16 = jnp.bfloat16
F32 = jnp.float32
POOL_VMEM = 60 * 1024 * 1024
LOSS_VMEM = 24 * 1024 * 1024
GRAM_VMEM = 12 * 1024 * 1024
SIDE_VMEM = 12 * 1024 * 1024


def dot(a, b):
    return lax.dot_general(a, b, (((1,), (0,)), ((), ())), preferred_element_type=F32)


def dot_nt(a, b):
    return lax.dot_general(a, b, (((1,), (1,)), ((), ())), preferred_element_type=F32)


def dot_tn(a, b):
    return lax.dot_general(a, b, (((0,), (0,)), ((), ())), preferred_element_type=F32)


def rank_of():
    z, y, x, core = (lax.axis_index(a) for a in AXES)
    return ((z * 4 + y) * 4 + x) * 2 + core


def pool_kernel(
    seg_ref,
    counts_ref,
    positives_ref,
    x_hbm,
    wqkv_hbm,
    wout_hbm,
    gain_ref,
    out_ref,
    x_ref,
    wqkv_ref,
    wout_ref,
    q_ref,
    k_ref,
    v_ref,
    ctx_ref,
    sums_ref,
    sems,
    *,
    copies,
    tile,
):
    rows, width = x_ref.shape
    slots = out_ref.shape[1]
    hidden = HEADS * HEAD_DIM
    chunk = 256
    chunks = 3 * hidden // chunk

    x_copy = pltpu.make_async_copy(x_hbm, x_ref, sems.at[0])
    x_copy.start()
    w_copies = []
    for c in range(chunks):
        cols = slice(c * chunk, (c + 1) * chunk)
        w_copies.append(
            pltpu.make_async_copy(wqkv_hbm.at[:, cols], wqkv_ref.at[:, cols], sems.at[1 + c])
        )
        w_copies[-1].start()
    wout_copy = pltpu.make_async_copy(wout_hbm, wout_ref, sems.at[1 + chunks])
    wout_copy.start()

    seg = seg_ref[...]
    begins = [jnp.int32(0)]
    for s in range(1, slots):
        begins.append(jnp.sum((seg < s).astype(F32)).astype(jnp.int32))
    begins.append(jnp.int32(rows))

    row_id = lax.broadcasted_iota(jnp.int32, (rows, 2 * HEAD_DIM), 0)
    lane = lax.broadcasted_iota(jnp.int32, (rows, 2 * HEAD_DIM), 1)
    of_row = jnp.zeros((rows, 2 * HEAD_DIM), jnp.int32)
    for s in range(1, slots):
        of_row += (row_id >= begins[s]).astype(jnp.int32)
    feature = lane % HEAD_DIM
    mine = feature == of_row
    q_mark = jnp.where(mine, 1.0, 0.0).astype(BF16)
    k_mark = jnp.where(mine | (feature >= slots), 0.0, FAR).astype(BF16)
    first_half = lane < HEAD_DIM

    x_copy.wait()
    def project(kind, g, carry):
        c0 = pl.multiple_of(kind * hidden + g * chunk, chunk)
        part = dot(x_ref[...], wqkv_ref[:, pl.ds(c0, chunk)])
        if kind == 0:
            part = part * (LOG2E * HEAD_DIM**-0.5)
        part = part.astype(BF16)
        for p in range(chunk // (2 * HEAD_DIM)):
            pair = part[:, p * 2 * HEAD_DIM : (p + 1) * 2 * HEAD_DIM]
            head = g * (chunk // HEAD_DIM) + 2 * p
            if kind == 0:
                q_ref[head] = jnp.where(first_half, pair, q_mark)
                q_ref[head + 1] = jnp.where(first_half, q_mark, pair)
            elif kind == 1:
                k_ref[head] = jnp.where(first_half, pair, k_mark)
                k_ref[head + 1] = jnp.where(first_half, k_mark, pair)
            else:
                turned = pair.T
                for i in range(2):
                    v_ref[head + i, 0:HEAD_DIM, :] = turned[i * HEAD_DIM : (i + 1) * HEAD_DIM]
                    v_ref[head + i, HEAD_DIM:, :] = jnp.ones((ONES, rows), BF16)
        return carry

    for kind in range(3):
        for c in range(kind * chunks // 3, (kind + 1) * chunks // 3):
            w_copies[c].wait()
        lax.fori_loop(0, chunks // 3, functools.partial(project, kind), 0)

    wout_copy.wait()
    sums_ref[...] = jnp.zeros_like(sums_ref)
    ctx_ref[...] = jnp.zeros_like(ctx_ref)
    key_tile = 128
    key_tiles = rows // key_tile
    widths = [w for w in (3, 4, 5, 6, 8) if w <= key_tiles]

    def project_out(r0):
        return x_ref[pl.ds(r0, tile), :].astype(F32) + dot_tn(ctx_ref[...], wout_ref[...])

    def pool_tile(resid, r0, valid):
        centre = resid - jnp.mean(resid, axis=1, keepdims=True)
        variance = jnp.mean(centre * centre, axis=1, keepdims=True)
        out = (centre * lax.rsqrt(variance + 1e-05) * gain_ref[...]).astype(BF16)
        slot = lax.broadcasted_iota(jnp.int32, (16, tile), 0)
        token = lax.broadcasted_iota(jnp.int32, (16, tile), 1) + r0
        member = jnp.zeros((16, tile), jnp.bool_)
        for s in range(slots):
            member |= (slot == s) & (token >= begins[s]) & (token < begins[s + 1])
        member = jnp.where(member & valid, 1.0, 0.0).astype(BF16)
        sums_ref[...] += dot(member, out)

    def one_tile(t, carry):
        r0 = pl.multiple_of(t * tile, tile)
        last = pl.multiple_of(jnp.maximum(r0 - tile, 0), tile)
        low = jnp.int32(0)
        high = jnp.int32(rows)
        for s in range(1, slots):
            low = jnp.where(begins[s] <= r0, begins[s], low)
        for s in range(slots - 1, 0, -1):
            high = jnp.where(begins[s] >= r0 + tile, begins[s], high)
        k0 = low // key_tile
        need = (high + key_tile - 1) // key_tile - k0

        for i, w in enumerate(widths):
            above = widths[i - 1] if i else 0

            @pl.when((need > above) & (need <= w))
            def _():
                start = pl.multiple_of(jnp.minimum(k0, key_tiles - w) * key_tile, key_tile)
                def score(h):
                    q = q_ref[h, pl.ds(r0, tile), :]
                    k = k_ref[h, pl.ds(start, w * key_tile), :]
                    return dot_nt(k, q)

                def soften(s):
                    return jnp.exp2(s - jnp.max(s, axis=0, keepdims=True)).astype(BF16)

                def finish(h, e):
                    v = v_ref[h, :, pl.ds(start, w * key_tile)]
                    out = dot(v, e)
                    part = out[0:HEAD_DIM] / out[HEAD_DIM : HEAD_DIM + 1]
                    ctx_ref[h * HEAD_DIM : (h + 1) * HEAD_DIM, :] = part.astype(BF16)

                resid = project_out(last)
                ahead = [score(0), score(1)]
                for h in range(0, HEADS, 2):
                    now = ahead
                    if h + 2 < HEADS:
                        ahead = [score(h + 2), score(h + 3)]
                    es = [soften(s) for s in now]
                    for i in range(2):
                        finish(h + i, es[i])
                    if h == 2:
                        pool_tile(resid, last, t > 0)

        return carry

    lax.fori_loop(0, rows // tile, one_tile, 0)
    last = rows - tile
    pool_tile(project_out(last), last, True)

    slot_col = lax.broadcasted_iota(jnp.int32, (slots, 1), 0)
    sizes = jnp.ones((slots, 1), F32)
    for s in range(slots):
        sizes = jnp.where(slot_col == s, (begins[s + 1] - begins[s]).astype(F32), sizes)
    pooled = (sums_ref[0:slots, :] / sizes).astype(BF16)

    rank = rank_of()
    count = counts_ref[rank]
    line = lax.broadcasted_iota(jnp.int32, (slots, META), 0)
    col = lax.broadcasted_iota(jnp.int32, (slots, META), 1)
    positive = jnp.zeros((slots, META), jnp.int32)
    for s in range(slots):
        positive = jnp.where(line == s, positives_ref[s], positive)
    own = rank * slots + line
    meta = jnp.where(col == 0, positive >> 5, 0)
    meta = jnp.where(col == 1, positive & 31, meta)
    meta = jnp.where(col == 2, (line < count).astype(jnp.int32), meta)
    meta = jnp.where(col == 3, own >> 5, meta)
    meta = jnp.where(col == 4, own & 31, meta)
    meta = meta.astype(F32).astype(BF16)
    for i in range(copies):
        out_ref[i, :, 0:width] = pooled
        out_ref[i, :, width:] = meta


def pooled_rows(tokens, seg_ids, counts, positives, w_qkv, w_out, ln_gain, copies):
    rows, width = tokens.shape
    slots = positives.shape[0]
    hidden = w_out.shape[0]
    tile = 256
    any_spec = pl.BlockSpec(memory_space=pltpu.HBM)
    vmem = pl.BlockSpec(memory_space=pltpu.VMEM)
    smem = pl.BlockSpec(memory_space=pltpu.SMEM)
    return pl.pallas_call(
        functools.partial(pool_kernel, copies=copies, tile=tile),
        out_shape=jax.ShapeDtypeStruct((copies, slots, width + META), BF16),
        in_specs=[vmem, smem, smem, any_spec, any_spec, any_spec, vmem],
        out_specs=vmem,
        scratch_shapes=[
            pltpu.VMEM((rows, width), BF16),
            pltpu.VMEM((width, 3 * hidden), BF16),
            pltpu.VMEM((hidden, width), BF16),
            pltpu.VMEM((HEADS, rows, 2 * HEAD_DIM), BF16),
            pltpu.VMEM((HEADS, rows, 2 * HEAD_DIM), BF16),
            pltpu.VMEM((HEADS, HEAD_DIM + ONES, rows), BF16),
            pltpu.VMEM((hidden, tile), BF16),
            pltpu.VMEM((16, width), F32),
            pltpu.SemaphoreType.DMA((8,)),
        ],
        compiler_params=pltpu.CompilerParams(vmem_limit_bytes=POOL_VMEM),
        cost_estimate=pl.CostEstimate(
            flops=2 * rows * width * 4 * hidden + 4 * rows * rows * hidden,
            bytes_accessed=2 * (rows * width + 4 * width * hidden),
            transcendentals=HEADS * rows * rows // 2,
        ),
        name="pool",
    )(seg_ids, counts, positives, tokens, w_qkv, w_out, ln_gain.reshape(1, width))


def gram_kernel(w_ref, out_ref, *, block):
    for b in range(out_ref.shape[0] // block):
        right = w_ref[b * block : (b + 1) * block, :]
        for c in range(b + 1):
            left = w_ref[c * block : (c + 1) * block, :]
            value = dot_nt(left, right).astype(BF16)
            out_ref[c * block : (c + 1) * block, b * block : (b + 1) * block] = value
            if c < b:
                out_ref[b * block : (b + 1) * block, c * block : (c + 1) * block] = value.T


def gram_of(w_proj):
    rows, depth = w_proj.shape
    vmem = pl.BlockSpec(memory_space=pltpu.VMEM)
    return pl.pallas_call(
        functools.partial(gram_kernel, block=256),
        out_shape=jax.ShapeDtypeStruct((rows, rows), BF16),
        in_specs=[vmem],
        out_specs=vmem,
        compiler_params=pltpu.CompilerParams(vmem_limit_bytes=GRAM_VMEM),
        cost_estimate=pl.CostEstimate(
            flops=2 * rows * rows * depth, bytes_accessed=2 * rows * depth, transcendentals=0
        ),
        name="gram",
    )(w_proj)


def side_kernel(pooled_ref, gram_ref, left_ref, right_ref, norm_ref, *, block):
    sides(pooled_ref, gram_ref[...], left_ref, right_ref, norm_ref, 0, block)


def sides(pooled_ref, gram, left_ref, right_ref, norm_ref, place, block):
    width = gram.shape[0]
    for begin in range(0, pooled_ref.shape[0], block):
        rows = slice(place + begin, place + begin + block)
        pooled = pooled_ref[begin : begin + block, 0:width]
        through = dot(pooled, gram)
        wide = pooled.astype(F32)
        square = jnp.sum(through * wide, axis=1, keepdims=True)
        rnorm = lax.rsqrt(jnp.maximum(square, 0.0) + 1e-06)
        left_ref[rows, :] = (through * (rnorm * (LOGIT_SCALE * LOG2E))).astype(BF16)
        right_ref[rows, :] = (wide * rnorm).astype(BF16)
        norm_ref[rows, :] = jnp.broadcast_to(rnorm, (block, norm_ref.shape[1]))


def own_sides(mine, gram):
    part = mine.shape[0]
    width = gram.shape[0]
    vmem = pl.BlockSpec(memory_space=pltpu.VMEM)
    return pl.pallas_call(
        functools.partial(side_kernel, block=256),
        out_shape=(
            jax.ShapeDtypeStruct((part, width), BF16),
            jax.ShapeDtypeStruct((part, width), BF16),
            jax.ShapeDtypeStruct((part, 128), F32),
        ),
        in_specs=[vmem, vmem],
        out_specs=(vmem, vmem, vmem),
        compiler_params=pltpu.CompilerParams(vmem_limit_bytes=SIDE_VMEM),
        cost_estimate=pl.CostEstimate(
            flops=2 * part * width * width,
            bytes_accessed=8 * part * width,
            transcendentals=part,
        ),
        name="sides",
    )(mine, gram)


def loss_kernel(
    mine_ref,
    other_ref,
    gram_ref,
    own_left_ref,
    own_right_ref,
    own_norm_ref,
    loss_ref,
    grad_ref,
    left_ref,
    right_ref,
    logit_ref,
    norm_ref,
):
    total, width = right_ref.shape
    part = total // 2
    slots = grad_ref.shape[0]
    block = 256
    gram = gram_ref[...]

    right_ref[0:part, :] = own_right_ref[...]
    sides(other_ref, gram, left_ref, right_ref, norm_ref, part, block)

    meta = jnp.concatenate([mine_ref[:, width:], other_ref[:, width:]], axis=0)
    pick = lax.broadcasted_iota(jnp.int32, (16, META), 0) == lax.broadcasted_iota(
        jnp.int32, (16, META), 1
    )
    lines = dot_nt(pick.astype(F32).astype(BF16), meta)
    spread = (lax.broadcasted_iota(jnp.int32, (META, 128), 0) == 2).astype(F32).astype(BF16)
    live_col = dot(meta, spread)

    right = right_ref[...]
    sums = jnp.zeros((8, total), F32)
    for b in range(total // block):
        rows = slice(b * block, (b + 1) * block)
        left = own_left_ref[rows, :] if b * block < part else left_ref[rows, :]
        logit = dot_nt(left, right)
        logit_ref[rows, :] = logit
        live = live_col[rows, :]
        pieces = []
        for c in range(total // 128):
            term = jnp.exp2(logit[:, c * 128 : (c + 1) * 128]) * live
            if b * block <= c * 128 < (b + 1) * block:
                row = lax.broadcasted_iota(jnp.int32, (block, 128), 0) + b * block
                col = lax.broadcasted_iota(jnp.int32, (block, 128), 1) + c * 128
                term = jnp.where(row == col, 0.0, term)
            pieces.append(jnp.sum(term.reshape(block // 8, 8, 128), axis=0))
        sums = sums + jnp.concatenate(pieces, axis=1)
    denominator_line = jnp.sum(sums, axis=0, keepdims=True)

    z, y, x, _ = (lax.axis_index(a) for a in AXES)
    begin = ((y * 4 + x) * 8 + z) * slots
    base = pl.multiple_of(begin // 16 * 16, 16)
    within = begin - base
    own_meta = mine_ref[pl.ds(base, 16), width:].astype(F32)
    own_positive = own_meta[:, 0:1] * 32.0 + own_meta[:, 1:2]
    own_live = own_meta[:, 2:3] > 0.5
    own_slot = own_meta[:, 3:4] * 32.0 + own_meta[:, 4:5]
    positive_line = lines[0:1, :] * 32.0 + lines[1:2, :]
    live_line = lines[2:3, :] > 0.5
    slot_line = lines[3:4, :] * 32.0 + lines[4:5, :]

    logit = logit_ref[pl.ds(base, 16), :]
    same = slot_line == own_slot
    raw = jnp.where(same, 0.0, jnp.exp2(logit))
    as_query = jnp.where(live_line, raw, 0.0)
    denominator = jnp.sum(as_query, axis=1, keepdims=True)
    target = slot_line == own_positive
    picked = jnp.sum(jnp.where(target, logit, 0.0), axis=1, keepdims=True) * (1.0 / LOG2E)
    loss = jnp.where(own_live, jnp.log(denominator) - picked, 0.0)
    for s in range(slots):
        row = lax.broadcasted_iota(jnp.int32, (16, 1), 0)
        loss_ref[s] = jnp.sum(jnp.where(row == within + s, loss, 0.0))
    query_weights = jnp.where(own_live, as_query / denominator - target.astype(F32), 0.0)
    hits = (positive_line == own_slot).astype(F32)
    key_weights = jnp.where(
        live_line, jnp.where(own_live, raw, 0.0) / denominator_line - hits, 0.0
    )
    weights = (query_weights + key_weights).astype(BF16)
    mix = dot(weights, right)
    image = dot(mix.astype(BF16), gram) * LOGIT_SCALE
    unit_image = own_left_ref[pl.ds(base, 16), :].astype(F32) * (1.0 / (LOGIT_SCALE * LOG2E))
    radial = LOGIT_SCALE * jnp.sum(mix * unit_image, axis=1, keepdims=True)
    rnorm = own_norm_ref[pl.ds(base, 16), 0:1]
    grad = (image - radial * unit_image) * rnorm
    out = grad[0:slots]
    for i in range(1, 16 // slots):
        out = jnp.where(within == i * slots, grad[i * slots : (i + 1) * slots], out)
    grad_ref[...] = out


def loss_and_grad(mine, other, gram, own, slots):
    part, padded = mine.shape
    width = padded - META
    total = 2 * part
    vmem = pl.BlockSpec(memory_space=pltpu.VMEM)
    return pl.pallas_call(
        loss_kernel,
        out_shape=(
            jax.ShapeDtypeStruct((slots,), F32),
            jax.ShapeDtypeStruct((slots, width), F32),
        ),
        in_specs=[vmem] * 6,
        out_specs=(pl.BlockSpec(memory_space=pltpu.SMEM), vmem),
        scratch_shapes=[
            pltpu.VMEM((total, width), BF16),
            pltpu.VMEM((total, width), BF16),
            pltpu.VMEM((total, total), F32),
            pltpu.VMEM((total, 128), F32),
        ],
        compiler_params=pltpu.CompilerParams(vmem_limit_bytes=LOSS_VMEM),
        cost_estimate=pl.CostEstimate(
            flops=4 * total * total * width,
            bytes_accessed=4 * total * width,
            transcendentals=total * total,
        ),
        name="loss",
    )(mine, other, gram, *own)


def body(tokens, seg_ids, counts, positives, w_qkv, w_out, ln_gain, w_proj):
    slots = positives.shape[0]
    z_size = lax.axis_size("dp_0")
    plane = ("dp_1", "dp_2")
    plane_size = lax.axis_size(plane)
    packed = pooled_rows(tokens, seg_ids, counts, positives, w_qkv, w_out, ln_gain, z_size)
    padded = packed.shape[-1]
    w_proj, packed = lax.optimization_barrier((w_proj, packed))
    gram = gram_of(w_proj)
    line = lax.all_to_all(packed, "dp_0", split_axis=0, concat_axis=0, tiled=True)
    line = line.reshape(z_size * slots, padded)
    line, gram = lax.optimization_barrier((line, gram))
    copies = jnp.broadcast_to(line, (plane_size, *line.shape))
    mine = lax.all_to_all(copies, plane, split_axis=0, concat_axis=0, tiled=True)
    mine = mine.reshape(plane_size * z_size * slots, padded)
    other = lax.ppermute(mine, "dp_3", [(0, 1), (1, 0)])
    own = own_sides(mine, gram)
    return loss_and_grad(mine, other, gram, own, slots)


def solution(mesh):
    finer = Mesh(mesh.devices.reshape(8, 4, 4, 2), AXES)
    return jax.shard_map(
        body,
        mesh=finer,
        in_specs=(P(AXES, None), P(AXES, None), P(), P(AXES), P(), P(), P(), P()),
        out_specs=(P(AXES), P(AXES, None)),
        check_vma=False,
    )
```

```python
import functools
import math

import jax
import jax.numpy as jnp
from jax import lax
from jax.experimental import pallas as pl
from jax.experimental.pallas import tpu as pltpu
from jax.sharding import Mesh
from jax.sharding import PartitionSpec as P

AXES = ("dp_0", "dp_1", "dp_2", "dp_3")
HEADS = 8
HEAD_DIM = 64
PAIRS = HEADS // 2
LOG2E = math.log2(math.e)
LOGIT_SCALE = 20.0
META = 128
ONES = 16
FAR = -1e30
BF16 = jnp.bfloat16
F32 = jnp.float32
POOL_VMEM = 60 * 1024 * 1024
LOSS_VMEM = 24 * 1024 * 1024
GRAM_VMEM = 12 * 1024 * 1024
SIDE_VMEM = 12 * 1024 * 1024


def dot(a, b):
    return lax.dot_general(a, b, (((1,), (0,)), ((), ())), preferred_element_type=F32)


def dot_nt(a, b):
    return lax.dot_general(a, b, (((1,), (1,)), ((), ())), preferred_element_type=F32)


def dot_tn(a, b):
    return lax.dot_general(a, b, (((0,), (0,)), ((), ())), preferred_element_type=F32)


def rank_of():
    z, y, x, core = (lax.axis_index(a) for a in AXES)
    return ((z * 4 + y) * 4 + x) * 2 + core


def pool_kernel(
    seg_ref,
    counts_ref,
    positives_ref,
    x_hbm,
    wqkv_hbm,
    wout_hbm,
    gain_ref,
    out_ref,
    x_ref,
    wqkv_ref,
    wout_ref,
    q_ref,
    k_ref,
    v_ref,
    ctx_ref,
    sums_ref,
    sems,
    *,
    copies,
    tile,
):
    rows, width = x_ref.shape
    slots = out_ref.shape[1]
    hidden = HEADS * HEAD_DIM
    chunk = 512
    chunks = 3 * hidden // chunk

    parts = 2
    x_copies = []
    for r in range(parts):
        some = slice(r * rows // parts, (r + 1) * rows // parts)
        x_copies.append(
            pltpu.make_async_copy(x_hbm.at[some, :], x_ref.at[some, :], sems.at[r])
        )
    w_copies = []
    for c in range(chunks):
        cols = slice(c * chunk, (c + 1) * chunk)
        w_copies.append(
            pltpu.make_async_copy(wqkv_hbm.at[:, cols], wqkv_ref.at[:, cols], sems.at[parts + c])
        )
    wout_copy = pltpu.make_async_copy(wout_hbm, wout_ref, sems.at[parts + chunks])
    for copy in [w_copies[0], *x_copies, *w_copies[1:], wout_copy]:
        copy.start()

    seg = seg_ref[...]
    begins = [jnp.int32(0)]
    for s in range(1, slots):
        begins.append(jnp.sum((seg < s).astype(F32)).astype(jnp.int32))
    begins.append(jnp.int32(rows))

    row_id = lax.broadcasted_iota(jnp.int32, (rows, 2 * HEAD_DIM), 0)
    lane = lax.broadcasted_iota(jnp.int32, (rows, 2 * HEAD_DIM), 1)
    of_row = jnp.zeros((rows, 2 * HEAD_DIM), jnp.int32)
    for s in range(1, slots):
        of_row += (row_id >= begins[s]).astype(jnp.int32)
    feature = lane % HEAD_DIM
    mine = feature == of_row
    q_mark = jnp.where(mine, 1.0, 0.0).astype(BF16)
    k_mark = jnp.where(mine | (feature >= slots), 0.0, FAR).astype(BF16)
    first_half = lane < HEAD_DIM

    def project(kind, some, g, carry):
        c0 = pl.multiple_of(kind * hidden + g * chunk, chunk)
        part = dot(x_ref[some, :], wqkv_ref[:, pl.ds(c0, chunk)])
        if kind == 0:
            part = part * (LOG2E * HEAD_DIM**-0.5)
        part = part.astype(BF16)
        left = first_half[some]
        for p in range(chunk // (2 * HEAD_DIM)):
            pair = part[:, p * 2 * HEAD_DIM : (p + 1) * 2 * HEAD_DIM]
            head = g * (chunk // HEAD_DIM) + 2 * p
            if kind == 0:
                q_ref[head, some, :] = jnp.where(left, pair, q_mark[some])
                q_ref[head + 1, some, :] = jnp.where(left, q_mark[some], pair)
            elif kind == 1:
                k_ref[head, some, :] = jnp.where(left, pair, k_mark[some])
                k_ref[head + 1, some, :] = jnp.where(left, k_mark[some], pair)
            else:
                turned = pair.T
                for i in range(2):
                    v_ref[head + i, 0:HEAD_DIM, some] = turned[i * HEAD_DIM : (i + 1) * HEAD_DIM]
                    v_ref[head + i, HEAD_DIM:, some] = jnp.ones((ONES, turned.shape[1]), BF16)
        return carry

    w_copies[0].wait()
    for r in range(parts):
        x_copies[r].wait()
        project(0, slice(r * rows // parts, (r + 1) * rows // parts), 0, 0)
    for kind in (1, 2):
        w_copies[kind].wait()
        for r in range(parts):
            project(kind, slice(r * rows // parts, (r + 1) * rows // parts), 0, 0)

    wout_copy.wait()
    sums_ref[...] = jnp.zeros_like(sums_ref)
    ctx_ref[...] = jnp.zeros_like(ctx_ref)
    key_tile = 128
    key_tiles = rows // key_tile
    widths = [w for w in (3, 4, 5, 6, 8) if w <= key_tiles]

    def project_out(r0):
        return x_ref[pl.ds(r0, tile), :].astype(F32) + dot_tn(ctx_ref[...], wout_ref[...])

    def pool_tile(resid, r0, valid):
        centre = resid - jnp.mean(resid, axis=1, keepdims=True)
        variance = jnp.mean(centre * centre, axis=1, keepdims=True)
        out = (centre * lax.rsqrt(variance + 1e-05) * gain_ref[...]).astype(BF16)
        slot = lax.broadcasted_iota(jnp.int32, (16, tile), 0)
        token = lax.broadcasted_iota(jnp.int32, (16, tile), 1) + r0
        member = jnp.zeros((16, tile), jnp.bool_)
        for s in range(slots):
            member |= (slot == s) & (token >= begins[s]) & (token < begins[s + 1])
        member = jnp.where(member & valid, 1.0, 0.0).astype(BF16)
        sums_ref[...] += dot(member, out)

    def one_tile(t, carry):
        r0 = pl.multiple_of(t * tile, tile)
        last = pl.multiple_of(jnp.maximum(r0 - tile, 0), tile)
        low = jnp.int32(0)
        high = jnp.int32(rows)
        for s in range(1, slots):
            low = jnp.where(begins[s] <= r0, begins[s], low)
        for s in range(slots - 1, 0, -1):
            high = jnp.where(begins[s] >= r0 + tile, begins[s], high)
        k0 = low // key_tile
        need = (high + key_tile - 1) // key_tile - k0

        for i, w in enumerate(widths):
            above = widths[i - 1] if i else 0

            @pl.when((need > above) & (need <= w))
            def _():
                start = pl.multiple_of(jnp.minimum(k0, key_tiles - w) * key_tile, key_tile)
                def score(h):
                    q = q_ref[h, pl.ds(r0, tile), :]
                    k = k_ref[h, pl.ds(start, w * key_tile), :]
                    return dot_nt(k, q)

                def soften(s):
                    return jnp.exp2(s - jnp.max(s, axis=0, keepdims=True)).astype(BF16)

                def finish(h, e):
                    v = v_ref[h, :, pl.ds(start, w * key_tile)]
                    out = dot(v, e)
                    part = out[0:HEAD_DIM] / out[HEAD_DIM : HEAD_DIM + 1]
                    ctx_ref[h * HEAD_DIM : (h + 1) * HEAD_DIM, :] = part.astype(BF16)

                resid = project_out(last)
                scores = [score(h) for h in range(4)]
                soft = []
                for h in range(HEADS):
                    if h + 4 < HEADS:
                        scores.append(score(h + 4))
                    soft.append(soften(scores[h]))
                    if h >= 2:
                        finish(h - 2, soft[h - 2])
                    if h == 2:
                        pool_tile(resid, last, t > 0)
                for h in range(HEADS - 2, HEADS):
                    finish(h, soft[h])

        return carry

    lax.fori_loop(0, rows // tile, one_tile, 0)
    last = rows - tile
    pool_tile(project_out(last), last, True)

    slot_col = lax.broadcasted_iota(jnp.int32, (slots, 1), 0)
    sizes = jnp.ones((slots, 1), F32)
    for s in range(slots):
        sizes = jnp.where(slot_col == s, (begins[s + 1] - begins[s]).astype(F32), sizes)
    pooled = (sums_ref[0:slots, :] / sizes).astype(BF16)

    rank = rank_of()
    count = counts_ref[rank]
    line = lax.broadcasted_iota(jnp.int32, (slots, META), 0)
    col = lax.broadcasted_iota(jnp.int32, (slots, META), 1)
    positive = jnp.zeros((slots, META), jnp.int32)
    for s in range(slots):
        positive = jnp.where(line == s, positives_ref[s], positive)
    own = rank * slots + line
    meta = jnp.where(col == 0, positive >> 5, 0)
    meta = jnp.where(col == 1, positive & 31, meta)
    meta = jnp.where(col == 2, (line < count).astype(jnp.int32), meta)
    meta = jnp.where(col == 3, own >> 5, meta)
    meta = jnp.where(col == 4, own & 31, meta)
    meta = meta.astype(F32).astype(BF16)
    for i in range(copies):
        out_ref[i, :, 0:width] = pooled
        out_ref[i, :, width:] = meta


def pooled_rows(tokens, seg_ids, counts, positives, w_qkv, w_out, ln_gain, copies):
    rows, width = tokens.shape
    slots = positives.shape[0]
    hidden = w_out.shape[0]
    tile = 256
    any_spec = pl.BlockSpec(memory_space=pltpu.HBM)
    vmem = pl.BlockSpec(memory_space=pltpu.VMEM)
    smem = pl.BlockSpec(memory_space=pltpu.SMEM)
    return pl.pallas_call(
        functools.partial(pool_kernel, copies=copies, tile=tile),
        out_shape=jax.ShapeDtypeStruct((copies, slots, width + META), BF16),
        in_specs=[vmem, smem, smem, any_spec, any_spec, any_spec, vmem],
        out_specs=vmem,
        scratch_shapes=[
            pltpu.VMEM((rows, width), BF16),
            pltpu.VMEM((width, 3 * hidden), BF16),
            pltpu.VMEM((hidden, width), BF16),
            pltpu.VMEM((HEADS, rows, 2 * HEAD_DIM), BF16),
            pltpu.VMEM((HEADS, rows, 2 * HEAD_DIM), BF16),
            pltpu.VMEM((HEADS, HEAD_DIM + ONES, rows), BF16),
            pltpu.VMEM((hidden, tile), BF16),
            pltpu.VMEM((16, width), F32),
            pltpu.SemaphoreType.DMA((8,)),
        ],
        compiler_params=pltpu.CompilerParams(vmem_limit_bytes=POOL_VMEM),
        cost_estimate=pl.CostEstimate(
            flops=2 * rows * width * 4 * hidden + 4 * rows * rows * hidden,
            bytes_accessed=2 * (rows * width + 4 * width * hidden),
            transcendentals=HEADS * rows * rows // 2,
        ),
        name="pool",
    )(seg_ids, counts, positives, tokens, w_qkv, w_out, ln_gain.reshape(1, width))


def gram_kernel(w_ref, out_ref, *, block):
    for b in range(out_ref.shape[0] // block):
        right = w_ref[b * block : (b + 1) * block, :]
        for c in range(b + 1):
            left = w_ref[c * block : (c + 1) * block, :]
            value = dot_nt(left, right).astype(BF16)
            out_ref[c * block : (c + 1) * block, b * block : (b + 1) * block] = value
            if c < b:
                out_ref[b * block : (b + 1) * block, c * block : (c + 1) * block] = value.T


def gram_of(w_proj):
    rows, depth = w_proj.shape
    vmem = pl.BlockSpec(memory_space=pltpu.VMEM)
    return pl.pallas_call(
        functools.partial(gram_kernel, block=256),
        out_shape=jax.ShapeDtypeStruct((rows, rows), BF16),
        in_specs=[vmem],
        out_specs=vmem,
        compiler_params=pltpu.CompilerParams(vmem_limit_bytes=GRAM_VMEM),
        cost_estimate=pl.CostEstimate(
            flops=2 * rows * rows * depth, bytes_accessed=2 * rows * depth, transcendentals=0
        ),
        name="gram",
    )(w_proj)


def side_kernel(pooled_ref, gram_ref, left_ref, right_ref, norm_ref, *, block):
    sides(pooled_ref, gram_ref[...], left_ref, right_ref, norm_ref, 0, block)


def sides(pooled_ref, gram, left_ref, right_ref, norm_ref, place, block):
    width = gram.shape[0]
    for begin in range(0, pooled_ref.shape[0], block):
        rows = slice(place + begin, place + begin + block)
        pooled = pooled_ref[begin : begin + block, 0:width]
        through = dot(pooled, gram)
        wide = pooled.astype(F32)
        square = jnp.sum(through * wide, axis=1, keepdims=True)
        rnorm = lax.rsqrt(jnp.maximum(square, 0.0) + 1e-06)
        left_ref[rows, :] = (through * (rnorm * (LOGIT_SCALE * LOG2E))).astype(BF16)
        right_ref[rows, :] = (wide * rnorm).astype(BF16)
        norm_ref[rows, :] = jnp.broadcast_to(rnorm, (block, norm_ref.shape[1]))


def own_sides(mine, gram):
    part = mine.shape[0]
    width = gram.shape[0]
    vmem = pl.BlockSpec(memory_space=pltpu.VMEM)
    return pl.pallas_call(
        functools.partial(side_kernel, block=256),
        out_shape=(
            jax.ShapeDtypeStruct((part, width), BF16),
            jax.ShapeDtypeStruct((part, width), BF16),
            jax.ShapeDtypeStruct((part, 128), F32),
        ),
        in_specs=[vmem, vmem],
        out_specs=(vmem, vmem, vmem),
        compiler_params=pltpu.CompilerParams(vmem_limit_bytes=SIDE_VMEM),
        cost_estimate=pl.CostEstimate(
            flops=2 * part * width * width,
            bytes_accessed=8 * part * width,
            transcendentals=part,
        ),
        name="sides",
    )(mine, gram)


def loss_kernel(
    mine_ref,
    other_ref,
    gram_ref,
    own_left_ref,
    own_right_ref,
    own_norm_ref,
    loss_ref,
    grad_ref,
    left_ref,
    right_ref,
    logit_ref,
    norm_ref,
):
    total, width = right_ref.shape
    part = total // 2
    slots = grad_ref.shape[0]
    block = 256
    gram = gram_ref[...]

    right_ref[0:part, :] = own_right_ref[...]
    sides(other_ref, gram, left_ref, right_ref, norm_ref, part, block)

    meta = jnp.concatenate([mine_ref[:, width:], other_ref[:, width:]], axis=0)
    pick = lax.broadcasted_iota(jnp.int32, (16, META), 0) == lax.broadcasted_iota(
        jnp.int32, (16, META), 1
    )
    lines = dot_nt(pick.astype(F32).astype(BF16), meta)
    spread = (lax.broadcasted_iota(jnp.int32, (META, 128), 0) == 2).astype(F32).astype(BF16)
    live_col = dot(meta, spread)

    right = right_ref[...]
    sums = jnp.zeros((8, total), F32)
    for b in range(total // block):
        rows = slice(b * block, (b + 1) * block)
        left = own_left_ref[rows, :] if b * block < part else left_ref[rows, :]
        logit = dot_nt(left, right)
        logit_ref[rows, :] = logit
        live = live_col[rows, :]
        pieces = []
        for c in range(total // 128):
            term = jnp.exp2(logit[:, c * 128 : (c + 1) * 128]) * live
            if b * block <= c * 128 < (b + 1) * block:
                row = lax.broadcasted_iota(jnp.int32, (block, 128), 0) + b * block
                col = lax.broadcasted_iota(jnp.int32, (block, 128), 1) + c * 128
                term = jnp.where(row == col, 0.0, term)
            pieces.append(jnp.sum(term.reshape(block // 8, 8, 128), axis=0))
        sums = sums + jnp.concatenate(pieces, axis=1)
    denominator_line = jnp.sum(sums, axis=0, keepdims=True)

    z, y, x, _ = (lax.axis_index(a) for a in AXES)
    begin = ((y * 4 + x) * 8 + z) * slots
    base = pl.multiple_of(begin // 16 * 16, 16)
    within = begin - base
    own_meta = mine_ref[pl.ds(base, 16), width:].astype(F32)
    own_positive = own_meta[:, 0:1] * 32.0 + own_meta[:, 1:2]
    own_live = own_meta[:, 2:3] > 0.5
    own_slot = own_meta[:, 3:4] * 32.0 + own_meta[:, 4:5]
    positive_line = lines[0:1, :] * 32.0 + lines[1:2, :]
    live_line = lines[2:3, :] > 0.5
    slot_line = lines[3:4, :] * 32.0 + lines[4:5, :]

    logit = logit_ref[pl.ds(base, 16), :]
    same = slot_line == own_slot
    raw = jnp.where(same, 0.0, jnp.exp2(logit))
    as_query = jnp.where(live_line, raw, 0.0)
    denominator = jnp.sum(as_query, axis=1, keepdims=True)
    target = slot_line == own_positive
    picked = jnp.sum(jnp.where(target, logit, 0.0), axis=1, keepdims=True) * (1.0 / LOG2E)
    loss = jnp.where(own_live, jnp.log(denominator) - picked, 0.0)
    for s in range(slots):
        row = lax.broadcasted_iota(jnp.int32, (16, 1), 0)
        loss_ref[s] = jnp.sum(jnp.where(row == within + s, loss, 0.0))
    query_weights = jnp.where(own_live, as_query / denominator - target.astype(F32), 0.0)
    hits = (positive_line == own_slot).astype(F32)
    key_weights = jnp.where(
        live_line, jnp.where(own_live, raw, 0.0) / denominator_line - hits, 0.0
    )
    weights = (query_weights + key_weights).astype(BF16)
    mix = dot(weights, right)
    image = dot(mix.astype(BF16), gram) * LOGIT_SCALE
    unit_image = own_left_ref[pl.ds(base, 16), :].astype(F32) * (1.0 / (LOGIT_SCALE * LOG2E))
    radial = LOGIT_SCALE * jnp.sum(mix * unit_image, axis=1, keepdims=True)
    rnorm = own_norm_ref[pl.ds(base, 16), 0:1]
    grad = (image - radial * unit_image) * rnorm
    out = grad[0:slots]
    for i in range(1, 16 // slots):
        out = jnp.where(within == i * slots, grad[i * slots : (i + 1) * slots], out)
    grad_ref[...] = out


def loss_and_grad(mine, other, gram, own, slots):
    part, padded = mine.shape
    width = padded - META
    total = 2 * part
    vmem = pl.BlockSpec(memory_space=pltpu.VMEM)
    return pl.pallas_call(
        loss_kernel,
        out_shape=(
            jax.ShapeDtypeStruct((slots,), F32),
            jax.ShapeDtypeStruct((slots, width), F32),
        ),
        in_specs=[vmem] * 6,
        out_specs=(pl.BlockSpec(memory_space=pltpu.SMEM), vmem),
        scratch_shapes=[
            pltpu.VMEM((total, width), BF16),
            pltpu.VMEM((total, width), BF16),
            pltpu.VMEM((total, total), F32),
            pltpu.VMEM((total, 128), F32),
        ],
        compiler_params=pltpu.CompilerParams(vmem_limit_bytes=LOSS_VMEM),
        cost_estimate=pl.CostEstimate(
            flops=4 * total * total * width,
            bytes_accessed=4 * total * width,
            transcendentals=total * total,
        ),
        name="loss",
    )(mine, other, gram, *own)


def body(tokens, seg_ids, counts, positives, w_qkv, w_out, ln_gain, w_proj):
    slots = positives.shape[0]
    z_size = lax.axis_size("dp_0")
    plane = ("dp_1", "dp_2")
    plane_size = lax.axis_size(plane)
    packed = pooled_rows(tokens, seg_ids, counts, positives, w_qkv, w_out, ln_gain, z_size)
    padded = packed.shape[-1]
    w_proj, packed = lax.optimization_barrier((w_proj, packed))
    gram = gram_of(w_proj)
    line = lax.all_to_all(packed, "dp_0", split_axis=0, concat_axis=0, tiled=True)
    line = line.reshape(z_size * slots, padded)
    line, gram = lax.optimization_barrier((line, gram))
    copies = jnp.broadcast_to(line, (plane_size, *line.shape))
    mine = lax.all_to_all(copies, plane, split_axis=0, concat_axis=0, tiled=True)
    mine = mine.reshape(plane_size * z_size * slots, padded)
    other = lax.ppermute(mine, "dp_3", [(0, 1), (1, 0)])
    own = own_sides(mine, gram)
    return loss_and_grad(mine, other, gram, own, slots)


def solution(mesh):
    finer = Mesh(mesh.devices.reshape(8, 4, 4, 2), AXES)
    return jax.shard_map(
        body,
        mesh=finer,
        in_specs=(P(AXES, None), P(AXES, None), P(), P(AXES), P(), P(), P(), P()),
        out_specs=(P(AXES), P(AXES, None)),
        check_vma=False,
    )
```

```python
import functools
import math

import jax
import jax.numpy as jnp
from jax import lax
from jax.experimental import pallas as pl
from jax.experimental.pallas import tpu as pltpu
from jax.sharding import Mesh
from jax.sharding import PartitionSpec as P

AXES = ("dp_0", "dp_1", "dp_2", "dp_3")
HEADS = 8
HEAD_DIM = 64
PAIRS = HEADS // 2
LOG2E = math.log2(math.e)
LOGIT_SCALE = 20.0
META = 128
ONES = 16
FAR = -1e30
BF16 = jnp.bfloat16
F32 = jnp.float32
POOL_VMEM = 60 * 1024 * 1024
LOSS_VMEM = 24 * 1024 * 1024
GRAM_VMEM = 12 * 1024 * 1024
SIDE_VMEM = 12 * 1024 * 1024


def dot(a, b):
    return lax.dot_general(a, b, (((1,), (0,)), ((), ())), preferred_element_type=F32)


def dot_nt(a, b):
    return lax.dot_general(a, b, (((1,), (1,)), ((), ())), preferred_element_type=F32)


def dot_tn(a, b):
    return lax.dot_general(a, b, (((0,), (0,)), ((), ())), preferred_element_type=F32)


def rank_of():
    z, y, x, core = (lax.axis_index(a) for a in AXES)
    return ((z * 4 + y) * 4 + x) * 2 + core


def pool_kernel(
    seg_ref,
    counts_ref,
    positives_ref,
    x_hbm,
    wqkv_hbm,
    wout_hbm,
    gain_ref,
    out_ref,
    x_ref,
    wqkv_ref,
    wout_ref,
    q_ref,
    k_ref,
    v_ref,
    ctx_ref,
    sums_ref,
    sems,
    *,
    copies,
    tile,
):
    rows, width = x_ref.shape
    slots = out_ref.shape[1]
    hidden = HEADS * HEAD_DIM
    chunk = 512
    chunks = 3 * hidden // chunk

    parts = 2
    x_copies = []
    for r in range(parts):
        some = slice(r * rows // parts, (r + 1) * rows // parts)
        x_copies.append(
            pltpu.make_async_copy(x_hbm.at[some, :], x_ref.at[some, :], sems.at[r])
        )
    w_copies = []
    for c in range(chunks):
        cols = slice(c * chunk, (c + 1) * chunk)
        w_copies.append(
            pltpu.make_async_copy(wqkv_hbm.at[:, cols], wqkv_ref.at[:, cols], sems.at[parts + c])
        )
    wout_copy = pltpu.make_async_copy(wout_hbm, wout_ref, sems.at[parts + chunks])
    for copy in [w_copies[0], *x_copies, *w_copies[1:], wout_copy]:
        copy.start()

    seg = seg_ref[...]
    begins = [jnp.int32(0)]
    for s in range(1, slots):
        begins.append(jnp.sum((seg < s).astype(F32)).astype(jnp.int32))
    begins.append(jnp.int32(rows))

    row_id = lax.broadcasted_iota(jnp.int32, (rows, 2 * HEAD_DIM), 0)
    lane = lax.broadcasted_iota(jnp.int32, (rows, 2 * HEAD_DIM), 1)
    of_row = jnp.zeros((rows, 2 * HEAD_DIM), jnp.int32)
    for s in range(1, slots):
        of_row += (row_id >= begins[s]).astype(jnp.int32)
    feature = lane % HEAD_DIM
    mine = feature == of_row
    q_mark = jnp.where(mine, 1.0, 0.0).astype(BF16)
    k_mark = jnp.where(mine | (feature >= slots), 0.0, FAR).astype(BF16)
    first_half = lane < HEAD_DIM

    def product(kind, some):
        return dot(x_ref[some, :], wqkv_ref[:, kind * hidden : (kind + 1) * hidden])

    def place(kind, some, part):
        if kind == 0:
            part = part * (LOG2E * HEAD_DIM**-0.5)
        part = part.astype(BF16)
        left = first_half[some]
        for p in range(PAIRS):
            pair = part[:, p * 2 * HEAD_DIM : (p + 1) * 2 * HEAD_DIM]
            head = 2 * p
            if kind == 0:
                q_ref[head, some, :] = jnp.where(left, pair, q_mark[some])
                q_ref[head + 1, some, :] = jnp.where(left, q_mark[some], pair)
            elif kind == 1:
                k_ref[head, some, :] = jnp.where(left, pair, k_mark[some])
                k_ref[head + 1, some, :] = jnp.where(left, k_mark[some], pair)
            else:
                turned = pair.T
                for i in range(2):
                    v_ref[head + i, 0:HEAD_DIM, some] = turned[i * HEAD_DIM : (i + 1) * HEAD_DIM]
                    v_ref[head + i, HEAD_DIM:, some] = jnp.ones((ONES, turned.shape[1]), BF16)

    def in_turn(steps):
        ahead = product(*steps[0])
        for i, step in enumerate(steps):
            part = ahead
            if i + 1 < len(steps):
                ahead = product(*steps[i + 1])
            place(*step, part)

    pieces = [slice(r * rows // parts, (r + 1) * rows // parts) for r in range(parts)]
    w_copies[0].wait()
    for r in range(parts):
        x_copies[r].wait()
        in_turn([(0, pieces[r])])
    w_copies[1].wait()
    w_copies[2].wait()
    in_turn([(kind, some) for kind in (1, 2) for some in pieces])

    wout_copy.wait()
    sums_ref[...] = jnp.zeros_like(sums_ref)
    ctx_ref[...] = jnp.zeros_like(ctx_ref)
    key_tile = 128
    key_tiles = rows // key_tile
    widths = [w for w in (3, 4, 5, 6, 8) if w <= key_tiles]

    def project_out(r0):
        return x_ref[pl.ds(r0, tile), :].astype(F32) + dot_tn(ctx_ref[...], wout_ref[...])

    def pool_tile(resid, r0, valid):
        centre = resid - jnp.mean(resid, axis=1, keepdims=True)
        variance = jnp.mean(centre * centre, axis=1, keepdims=True)
        out = (centre * lax.rsqrt(variance + 1e-05) * gain_ref[...]).astype(BF16)
        slot = lax.broadcasted_iota(jnp.int32, (16, tile), 0)
        token = lax.broadcasted_iota(jnp.int32, (16, tile), 1) + r0
        member = jnp.zeros((16, tile), jnp.bool_)
        for s in range(slots):
            member |= (slot == s) & (token >= begins[s]) & (token < begins[s + 1])
        member = jnp.where(member & valid, 1.0, 0.0).astype(BF16)
        sums_ref[...] += dot(member, out)

    def one_tile(t, carry):
        r0 = pl.multiple_of(t * tile, tile)
        last = pl.multiple_of(jnp.maximum(r0 - tile, 0), tile)
        low = jnp.int32(0)
        high = jnp.int32(rows)
        for s in range(1, slots):
            low = jnp.where(begins[s] <= r0, begins[s], low)
        for s in range(slots - 1, 0, -1):
            high = jnp.where(begins[s] >= r0 + tile, begins[s], high)
        k0 = low // key_tile
        need = (high + key_tile - 1) // key_tile - k0

        for i, w in enumerate(widths):
            above = widths[i - 1] if i else 0

            @pl.when((need > above) & (need <= w))
            def _():
                start = pl.multiple_of(jnp.minimum(k0, key_tiles - w) * key_tile, key_tile)
                def score(h):
                    q = q_ref[h, pl.ds(r0, tile), :]
                    k = k_ref[h, pl.ds(start, w * key_tile), :]
                    return dot_nt(k, q)

                def soften(s):
                    return jnp.exp2(s - jnp.max(s, axis=0, keepdims=True)).astype(BF16)

                def finish(h, e):
                    v = v_ref[h, :, pl.ds(start, w * key_tile)]
                    out = dot(v, e)
                    part = out[0:HEAD_DIM] / out[HEAD_DIM : HEAD_DIM + 1]
                    ctx_ref[h * HEAD_DIM : (h + 1) * HEAD_DIM, :] = part.astype(BF16)

                resid = project_out(last)
                scores = [score(h) for h in range(4)]
                soft = []
                for h in range(HEADS):
                    if h + 4 < HEADS:
                        scores.append(score(h + 4))
                    soft.append(soften(scores[h]))
                    if h >= 2:
                        finish(h - 2, soft[h - 2])
                    if h == 2:
                        pool_tile(resid, last, t > 0)
                for h in range(HEADS - 2, HEADS):
                    finish(h, soft[h])

        return carry

    lax.fori_loop(0, rows // tile, one_tile, 0)
    last = rows - tile
    pool_tile(project_out(last), last, True)

    slot_col = lax.broadcasted_iota(jnp.int32, (slots, 1), 0)
    sizes = jnp.ones((slots, 1), F32)
    for s in range(slots):
        sizes = jnp.where(slot_col == s, (begins[s + 1] - begins[s]).astype(F32), sizes)
    pooled = (sums_ref[0:slots, :] / sizes).astype(BF16)

    rank = rank_of()
    count = counts_ref[rank]
    line = lax.broadcasted_iota(jnp.int32, (slots, META), 0)
    col = lax.broadcasted_iota(jnp.int32, (slots, META), 1)
    positive = jnp.zeros((slots, META), jnp.int32)
    for s in range(slots):
        positive = jnp.where(line == s, positives_ref[s], positive)
    own = rank * slots + line
    meta = jnp.where(col == 0, positive >> 5, 0)
    meta = jnp.where(col == 1, positive & 31, meta)
    meta = jnp.where(col == 2, (line < count).astype(jnp.int32), meta)
    meta = jnp.where(col == 3, own >> 5, meta)
    meta = jnp.where(col == 4, own & 31, meta)
    meta = meta.astype(F32).astype(BF16)
    for i in range(copies):
        out_ref[i, :, 0:width] = pooled
        out_ref[i, :, width:] = meta


def pooled_rows(tokens, seg_ids, counts, positives, w_qkv, w_out, ln_gain, copies):
    rows, width = tokens.shape
    slots = positives.shape[0]
    hidden = w_out.shape[0]
    tile = 256
    any_spec = pl.BlockSpec(memory_space=pltpu.HBM)
    vmem = pl.BlockSpec(memory_space=pltpu.VMEM)
    smem = pl.BlockSpec(memory_space=pltpu.SMEM)
    return pl.pallas_call(
        functools.partial(pool_kernel, copies=copies, tile=tile),
        out_shape=jax.ShapeDtypeStruct((copies, slots, width + META), BF16),
        in_specs=[vmem, smem, smem, any_spec, any_spec, any_spec, vmem],
        out_specs=vmem,
        scratch_shapes=[
            pltpu.VMEM((rows, width), BF16),
            pltpu.VMEM((width, 3 * hidden), BF16),
            pltpu.VMEM((hidden, width), BF16),
            pltpu.VMEM((HEADS, rows, 2 * HEAD_DIM), BF16),
            pltpu.VMEM((HEADS, rows, 2 * HEAD_DIM), BF16),
            pltpu.VMEM((HEADS, HEAD_DIM + ONES, rows), BF16),
            pltpu.VMEM((hidden, tile), BF16),
            pltpu.VMEM((16, width), F32),
            pltpu.SemaphoreType.DMA((8,)),
        ],
        compiler_params=pltpu.CompilerParams(vmem_limit_bytes=POOL_VMEM),
        cost_estimate=pl.CostEstimate(
            flops=2 * rows * width * 4 * hidden + 4 * rows * rows * hidden,
            bytes_accessed=2 * (rows * width + 4 * width * hidden),
            transcendentals=HEADS * rows * rows // 2,
        ),
        name="pool",
    )(seg_ids, counts, positives, tokens, w_qkv, w_out, ln_gain.reshape(1, width))


def gram_kernel(w_ref, out_ref, *, block):
    for b in range(out_ref.shape[0] // block):
        right = w_ref[b * block : (b + 1) * block, :]
        for c in range(b + 1):
            left = w_ref[c * block : (c + 1) * block, :]
            value = dot_nt(left, right).astype(BF16)
            out_ref[c * block : (c + 1) * block, b * block : (b + 1) * block] = value
            if c < b:
                out_ref[b * block : (b + 1) * block, c * block : (c + 1) * block] = value.T


def gram_of(w_proj):
    rows, depth = w_proj.shape
    vmem = pl.BlockSpec(memory_space=pltpu.VMEM)
    return pl.pallas_call(
        functools.partial(gram_kernel, block=256),
        out_shape=jax.ShapeDtypeStruct((rows, rows), BF16),
        in_specs=[vmem],
        out_specs=vmem,
        compiler_params=pltpu.CompilerParams(vmem_limit_bytes=GRAM_VMEM),
        cost_estimate=pl.CostEstimate(
            flops=2 * rows * rows * depth, bytes_accessed=2 * rows * depth, transcendentals=0
        ),
        name="gram",
    )(w_proj)


def live_spread(meta):
    pick = lax.broadcasted_iota(jnp.int32, (META, 128), 0) == 2
    return dot(meta, pick.astype(F32).astype(BF16))


def column_sums(logit, live, shift):
    rows, columns = logit.shape
    pieces = []
    for c in range(0, columns, 128):
        term = jnp.exp2(logit[:, c : c + 128]) * live
        if shift is not None and shift <= c < shift + rows:
            row = lax.broadcasted_iota(jnp.int32, (rows, 128), 0) + shift
            col = lax.broadcasted_iota(jnp.int32, (rows, 128), 1) + c
            term = jnp.where(row == col, 0.0, term)
        pieces.append(jnp.sum(term.reshape(rows // 8, 8, 128), axis=0))
    return jnp.concatenate(pieces, axis=1)


def own_place(slots):
    z, y, x, _ = (lax.axis_index(a) for a in AXES)
    begin = ((y * 4 + x) * 8 + z) * slots
    return begin, pl.multiple_of(begin // 16 * 16, 16)


def side_kernel(
    pooled_ref,
    gram_ref,
    left_ref,
    right_ref,
    norm_ref,
    line_ref,
    own_logit_ref,
    logit_ref,
    *,
    slots,
    block,
):
    part, width = left_ref.shape
    sides(pooled_ref, gram_ref[...], left_ref, right_ref, norm_ref, 0, block)
    live = live_spread(pooled_ref[:, width:])
    right = right_ref[...]
    sums = jnp.zeros((8, part), F32)
    for b in range(0, part, block):
        rows = slice(b, b + block)
        logit = dot_nt(left_ref[rows, :], right)
        logit_ref[rows, :] = logit
        sums = sums + column_sums(logit, live[rows], b)
    row = lax.broadcasted_iota(jnp.int32, (8, part), 0)
    norms = norm_ref[...].T[0:1]
    sums = jnp.sum(sums, axis=0, keepdims=True)
    line_ref[...] = jnp.where(row == 0, sums, jnp.where(row == 1, norms, 0.0))
    _, base = own_place(slots)
    own_logit_ref[...] = logit_ref[pl.ds(base, 16), :]


def sides(pooled_ref, gram, left_ref, right_ref, norm_ref, place, block):
    width = gram.shape[0]
    for begin in range(0, pooled_ref.shape[0], block):
        rows = slice(place + begin, place + begin + block)
        pooled = pooled_ref[begin : begin + block, 0:width]
        through = dot(pooled, gram)
        wide = pooled.astype(F32)
        square = jnp.sum(through * wide, axis=1, keepdims=True)
        rnorm = lax.rsqrt(jnp.maximum(square, 0.0) + 1e-06)
        left_ref[rows, :] = (through * (rnorm * (LOGIT_SCALE * LOG2E))).astype(BF16)
        right_ref[rows, :] = (wide * rnorm).astype(BF16)
        norm_ref[rows, :] = jnp.broadcast_to(rnorm, (block, norm_ref.shape[1]))


def own_sides(mine, gram, slots):
    part = mine.shape[0]
    width = gram.shape[0]
    vmem = pl.BlockSpec(memory_space=pltpu.VMEM)
    return pl.pallas_call(
        functools.partial(side_kernel, slots=slots, block=256),
        out_shape=(
            jax.ShapeDtypeStruct((part, width), BF16),
            jax.ShapeDtypeStruct((part, width), BF16),
            jax.ShapeDtypeStruct((part, 128), F32),
            jax.ShapeDtypeStruct((8, part), F32),
            jax.ShapeDtypeStruct((16, part), F32),
        ),
        in_specs=[vmem, vmem],
        out_specs=(vmem,) * 5,
        scratch_shapes=[pltpu.VMEM((part, part), F32)],
        compiler_params=pltpu.CompilerParams(vmem_limit_bytes=SIDE_VMEM),
        cost_estimate=pl.CostEstimate(
            flops=2 * part * width * (width + part),
            bytes_accessed=8 * part * width,
            transcendentals=part * part,
        ),
        name="sides",
    )(mine, gram)


def loss_kernel(
    mine_ref,
    other_ref,
    gram_ref,
    own_left_ref,
    own_right_ref,
    own_norm_ref,
    own_line_ref,
    own_logit_ref,
    far_line_ref,
    loss_ref,
    grad_ref,
    logit_ref,
):
    part, width = own_right_ref.shape
    slots = grad_ref.shape[0]
    block = 256

    meta = jnp.concatenate([mine_ref[:, width:], other_ref[:, width:]], axis=0)
    pick = lax.broadcasted_iota(jnp.int32, (16, META), 0) == lax.broadcasted_iota(
        jnp.int32, (16, META), 1
    )
    lines = dot_nt(pick.astype(F32).astype(BF16), meta)
    live = live_spread(mine_ref[:, width:])

    far = other_ref[:, 0:width]
    far_norm = far_line_ref[1:2, :]
    spread_norm = jnp.broadcast_to(far_norm, (block, part))
    far_live = jnp.broadcast_to(lines[2:3, part:], (block, part))
    far_sums = jnp.zeros((8, part), F32)
    row_sums = []
    raws = [dot_nt(own_left_ref[b : b + block, :], far) for b in range(0, part, block)]
    for i, raw in enumerate(raws):
        rows = slice(i * block, (i + 1) * block)
        logit = raw * spread_norm
        logit_ref[rows, :] = logit
        far_sums = far_sums + column_sums(logit, live[rows], None)
        row = jnp.sum(jnp.exp2(logit) * far_live, axis=1, keepdims=True)
        row_sums.append(jnp.broadcast_to(row, (block, 128)))
    own_line = own_line_ref[0:1, :] + jnp.concatenate(row_sums, axis=0).T[0:1]
    far_line = far_line_ref[0:1, :] + jnp.sum(far_sums, axis=0, keepdims=True)
    denominator_line = jnp.concatenate([own_line, far_line], axis=1)

    begin, base = own_place(slots)
    within = begin - base
    own_meta = mine_ref[pl.ds(base, 16), width:].astype(F32)
    own_positive = own_meta[:, 0:1] * 32.0 + own_meta[:, 1:2]
    own_live = own_meta[:, 2:3] > 0.5
    own_slot = own_meta[:, 3:4] * 32.0 + own_meta[:, 4:5]
    positive_line = lines[0:1, :] * 32.0 + lines[1:2, :]
    live_line = lines[2:3, :] > 0.5
    slot_line = lines[3:4, :] * 32.0 + lines[4:5, :]

    logit = jnp.concatenate([own_logit_ref[...], logit_ref[pl.ds(base, 16), :]], axis=1)
    same = slot_line == own_slot
    raw = jnp.where(same, 0.0, jnp.exp2(logit))
    as_query = jnp.where(live_line, raw, 0.0)
    denominator = jnp.sum(as_query, axis=1, keepdims=True)
    target = slot_line == own_positive
    picked = jnp.sum(jnp.where(target, logit, 0.0), axis=1, keepdims=True) * (1.0 / LOG2E)
    loss = jnp.where(own_live, jnp.log(denominator) - picked, 0.0)
    for s in range(slots):
        row = lax.broadcasted_iota(jnp.int32, (16, 1), 0)
        loss_ref[s] = jnp.sum(jnp.where(row == within + s, loss, 0.0))
    query_weights = jnp.where(own_live, as_query / denominator - target.astype(F32), 0.0)
    hits = (positive_line == own_slot).astype(F32)
    key_weights = jnp.where(
        live_line, jnp.where(own_live, raw, 0.0) / denominator_line - hits, 0.0
    )
    weights = query_weights + key_weights
    mix = dot(weights[:, 0:part].astype(BF16), own_right_ref[...])
    mix = mix + dot((weights[:, part:] * far_norm).astype(BF16), far)
    image = dot(mix.astype(BF16), gram_ref[...]) * LOGIT_SCALE
    unit_image = own_left_ref[pl.ds(base, 16), :].astype(F32) * (1.0 / (LOGIT_SCALE * LOG2E))
    radial = LOGIT_SCALE * jnp.sum(mix * unit_image, axis=1, keepdims=True)
    rnorm = own_norm_ref[pl.ds(base, 16), 0:1]
    grad = (image - radial * unit_image) * rnorm
    out = grad[0:slots]
    for i in range(1, 16 // slots):
        out = jnp.where(within == i * slots, grad[i * slots : (i + 1) * slots], out)
    grad_ref[...] = out


def loss_and_grad(mine, other, gram, own, far_line, slots):
    part, padded = mine.shape
    width = padded - META
    vmem = pl.BlockSpec(memory_space=pltpu.VMEM)
    return pl.pallas_call(
        loss_kernel,
        out_shape=(
            jax.ShapeDtypeStruct((slots,), F32),
            jax.ShapeDtypeStruct((slots, width), F32),
        ),
        in_specs=[vmem] * 9,
        out_specs=(pl.BlockSpec(memory_space=pltpu.SMEM), vmem),
        scratch_shapes=[pltpu.VMEM((part, part), F32)],
        compiler_params=pltpu.CompilerParams(vmem_limit_bytes=LOSS_VMEM),
        cost_estimate=pl.CostEstimate(
            flops=2 * part * part * width,
            bytes_accessed=8 * part * width,
            transcendentals=part * part,
        ),
        name="loss",
    )(mine, other, gram, *own, far_line)


def body(tokens, seg_ids, counts, positives, w_qkv, w_out, ln_gain, w_proj):
    slots = positives.shape[0]
    z_size = lax.axis_size("dp_0")
    plane = ("dp_1", "dp_2")
    plane_size = lax.axis_size(plane)
    packed = pooled_rows(tokens, seg_ids, counts, positives, w_qkv, w_out, ln_gain, z_size)
    padded = packed.shape[-1]
    w_proj, packed = lax.optimization_barrier((w_proj, packed))
    gram = gram_of(w_proj)
    line = lax.all_to_all(packed, "dp_0", split_axis=0, concat_axis=0, tiled=True)
    line = line.reshape(z_size * slots, padded)
    line, gram = lax.optimization_barrier((line, gram))
    copies = jnp.broadcast_to(line, (plane_size, *line.shape))
    mine = lax.all_to_all(copies, plane, split_axis=0, concat_axis=0, tiled=True)
    mine = mine.reshape(plane_size * z_size * slots, padded)
    pairs = [(0, 1), (1, 0)]
    other = lax.ppermute(mine, "dp_3", pairs)
    own = own_sides(mine, gram, slots)
    far_line = lax.ppermute(own[3], "dp_3", pairs)
    return loss_and_grad(mine, other, gram, own, far_line, slots)


def solution(mesh):
    finer = Mesh(mesh.devices.reshape(8, 4, 4, 2), AXES)
    return jax.shard_map(
        body,
        mesh=finer,
        in_specs=(P(AXES, None), P(AXES, None), P(), P(AXES), P(), P(), P(), P()),
        out_specs=(P(AXES), P(AXES, None)),
        check_vma=False,
    )
```

```python
import functools
import math

import jax
import jax.numpy as jnp
from jax import lax
from jax.experimental import pallas as pl
from jax.experimental.pallas import tpu as pltpu
from jax.sharding import Mesh
from jax.sharding import PartitionSpec as P

AXES = ("dp_0", "dp_1", "dp_2", "dp_3")
HEADS = 8
HEAD_DIM = 64
PAIRS = HEADS // 2
LOG2E = math.log2(math.e)
LOGIT_SCALE = 20.0
META = 128
ONES = 16
FAR = -1e30
BF16 = jnp.bfloat16
F32 = jnp.float32
POOL_VMEM = 60 * 1024 * 1024
LOSS_VMEM = 24 * 1024 * 1024
GRAM_VMEM = 57 * 1024 * 1024
SIDE_VMEM = 12 * 1024 * 1024


def dot(a, b):
    return lax.dot_general(a, b, (((1,), (0,)), ((), ())), preferred_element_type=F32)


def dot_nt(a, b):
    return lax.dot_general(a, b, (((1,), (1,)), ((), ())), preferred_element_type=F32)


def dot_tn(a, b):
    return lax.dot_general(a, b, (((0,), (0,)), ((), ())), preferred_element_type=F32)


def rank_of():
    z, y, x, core = (lax.axis_index(a) for a in AXES)
    return ((z * 4 + y) * 4 + x) * 2 + core


def pool_kernel(
    seg_ref,
    counts_ref,
    positives_ref,
    x_hbm,
    wqkv_hbm,
    wout_hbm,
    gain_ref,
    out_ref,
    x_ref,
    wqkv_ref,
    wout_ref,
    q_ref,
    k_ref,
    v_ref,
    ctx_ref,
    sums_ref,
    sems,
    *,
    copies,
    tile,
):
    rows, width = x_ref.shape
    slots = out_ref.shape[1]
    hidden = HEADS * HEAD_DIM
    chunk = 512
    chunks = 3 * hidden // chunk

    parts = 2
    x_copies = []
    for r in range(parts):
        some = slice(r * rows // parts, (r + 1) * rows // parts)
        x_copies.append(
            pltpu.make_async_copy(x_hbm.at[some, :], x_ref.at[some, :], sems.at[r])
        )
    w_copies = []
    for c in range(chunks):
        cols = slice(c * chunk, (c + 1) * chunk)
        w_copies.append(
            pltpu.make_async_copy(wqkv_hbm.at[:, cols], wqkv_ref.at[:, cols], sems.at[parts + c])
        )
    wout_copy = pltpu.make_async_copy(wout_hbm, wout_ref, sems.at[parts + chunks])
    for copy in [w_copies[0], *x_copies, *w_copies[1:], wout_copy]:
        copy.start()

    seg = seg_ref[...]
    begins = [jnp.int32(0)]
    for s in range(1, slots):
        begins.append(jnp.sum((seg < s).astype(F32)).astype(jnp.int32))
    begins.append(jnp.int32(rows))

    row_id = lax.broadcasted_iota(jnp.int32, (rows, 2 * HEAD_DIM), 0)
    lane = lax.broadcasted_iota(jnp.int32, (rows, 2 * HEAD_DIM), 1)
    of_row = jnp.zeros((rows, 2 * HEAD_DIM), jnp.int32)
    for s in range(1, slots):
        of_row += (row_id >= begins[s]).astype(jnp.int32)
    feature = lane % HEAD_DIM
    mine = feature == of_row
    q_mark = jnp.where(mine, 1.0, 0.0).astype(BF16)
    k_mark = jnp.where(mine | (feature >= slots), 0.0, FAR).astype(BF16)
    first_half = lane < HEAD_DIM

    def product(kind, some):
        return dot(x_ref[some, :], wqkv_ref[:, kind * hidden : (kind + 1) * hidden])

    def place(kind, some, part):
        if kind == 0:
            part = part * (LOG2E * HEAD_DIM**-0.5)
        part = part.astype(BF16)
        left = first_half[some]
        for p in range(PAIRS):
            pair = part[:, p * 2 * HEAD_DIM : (p + 1) * 2 * HEAD_DIM]
            head = 2 * p
            if kind == 0:
                q_ref[head, some, :] = jnp.where(left, pair, q_mark[some])
                q_ref[head + 1, some, :] = jnp.where(left, q_mark[some], pair)
            elif kind == 1:
                k_ref[head, some, :] = jnp.where(left, pair, k_mark[some])
                k_ref[head + 1, some, :] = jnp.where(left, k_mark[some], pair)
            else:
                turned = pair.T
                for i in range(2):
                    v_ref[head + i, 0:HEAD_DIM, some] = turned[i * HEAD_DIM : (i + 1) * HEAD_DIM]
                    v_ref[head + i, HEAD_DIM:, some] = jnp.ones((ONES, turned.shape[1]), BF16)

    def in_turn(steps):
        ahead = product(*steps[0])
        for i, step in enumerate(steps):
            part = ahead
            if i + 1 < len(steps):
                ahead = product(*steps[i + 1])
            place(*step, part)

    pieces = [slice(r * rows // parts, (r + 1) * rows // parts) for r in range(parts)]
    w_copies[0].wait()
    for r in range(parts):
        x_copies[r].wait()
        in_turn([(0, pieces[r])])
    w_copies[1].wait()
    w_copies[2].wait()
    in_turn([(kind, some) for kind in (1, 2) for some in pieces])

    wout_copy.wait()
    sums_ref[...] = jnp.zeros_like(sums_ref)
    ctx_ref[...] = jnp.zeros_like(ctx_ref)
    key_tile = 128
    key_tiles = rows // key_tile
    widths = [w for w in (3, 4, 5, 6, 8) if w <= key_tiles]

    def project_out(r0):
        return x_ref[pl.ds(r0, tile), :].astype(F32) + dot_tn(ctx_ref[...], wout_ref[...])

    def pool_tile(resid, r0, valid):
        centre = resid - jnp.mean(resid, axis=1, keepdims=True)
        variance = jnp.mean(centre * centre, axis=1, keepdims=True)
        out = (centre * lax.rsqrt(variance + 1e-05) * gain_ref[...]).astype(BF16)
        slot = lax.broadcasted_iota(jnp.int32, (16, tile), 0)
        token = lax.broadcasted_iota(jnp.int32, (16, tile), 1) + r0
        member = jnp.zeros((16, tile), jnp.bool_)
        for s in range(slots):
            member |= (slot == s) & (token >= begins[s]) & (token < begins[s + 1])
        member = jnp.where(member & valid, 1.0, 0.0).astype(BF16)
        sums_ref[...] += dot(member, out)

    def one_tile(t, carry):
        r0 = pl.multiple_of(t * tile, tile)
        last = pl.multiple_of(jnp.maximum(r0 - tile, 0), tile)
        low = jnp.int32(0)
        high = jnp.int32(rows)
        for s in range(1, slots):
            low = jnp.where(begins[s] <= r0, begins[s], low)
        for s in range(slots - 1, 0, -1):
            high = jnp.where(begins[s] >= r0 + tile, begins[s], high)
        k0 = low // key_tile
        need = (high + key_tile - 1) // key_tile - k0

        for i, w in enumerate(widths):
            above = widths[i - 1] if i else 0

            @pl.when((need > above) & (need <= w))
            def _():
                start = pl.multiple_of(jnp.minimum(k0, key_tiles - w) * key_tile, key_tile)
                def score(h):
                    q = q_ref[h, pl.ds(r0, tile), :]
                    k = k_ref[h, pl.ds(start, w * key_tile), :]
                    return dot_nt(k, q)

                def soften(s):
                    return jnp.exp2(s - jnp.max(s, axis=0, keepdims=True)).astype(BF16)

                def finish(h, e):
                    v = v_ref[h, :, pl.ds(start, w * key_tile)]
                    out = dot(v, e)
                    part = out[0:HEAD_DIM] / out[HEAD_DIM : HEAD_DIM + 1]
                    ctx_ref[h * HEAD_DIM : (h + 1) * HEAD_DIM, :] = part.astype(BF16)

                resid = project_out(last)
                scores = [score(h) for h in range(4)]
                soft = []
                for h in range(HEADS):
                    if h + 4 < HEADS:
                        scores.append(score(h + 4))
                    soft.append(soften(scores[h]))
                    if h >= 2:
                        finish(h - 2, soft[h - 2])
                    if h == 2:
                        pool_tile(resid, last, t > 0)
                for h in range(HEADS - 2, HEADS):
                    finish(h, soft[h])

        return carry

    lax.fori_loop(0, rows // tile, one_tile, 0)
    last = rows - tile
    pool_tile(project_out(last), last, True)

    slot_col = lax.broadcasted_iota(jnp.int32, (slots, 1), 0)
    sizes = jnp.ones((slots, 1), F32)
    for s in range(slots):
        sizes = jnp.where(slot_col == s, (begins[s + 1] - begins[s]).astype(F32), sizes)
    pooled = (sums_ref[0:slots, :] / sizes).astype(BF16)

    rank = rank_of()
    count = counts_ref[rank]
    line = lax.broadcasted_iota(jnp.int32, (slots, META), 0)
    col = lax.broadcasted_iota(jnp.int32, (slots, META), 1)
    positive = jnp.zeros((slots, META), jnp.int32)
    for s in range(slots):
        positive = jnp.where(line == s, positives_ref[s], positive)
    own = rank * slots + line
    meta = jnp.where(col == 0, positive >> 5, 0)
    meta = jnp.where(col == 1, positive & 31, meta)
    meta = jnp.where(col == 2, (line < count).astype(jnp.int32), meta)
    meta = jnp.where(col == 3, own >> 5, meta)
    meta = jnp.where(col == 4, own & 31, meta)
    meta = meta.astype(F32).astype(BF16)
    for i in range(copies):
        out_ref[i, :, 0:width] = pooled
        out_ref[i, :, width:] = meta


def pooled_rows(tokens, seg_ids, counts, positives, w_qkv, w_out, ln_gain, copies):
    rows, width = tokens.shape
    slots = positives.shape[0]
    hidden = w_out.shape[0]
    tile = 256
    any_spec = pl.BlockSpec(memory_space=pltpu.HBM)
    vmem = pl.BlockSpec(memory_space=pltpu.VMEM)
    smem = pl.BlockSpec(memory_space=pltpu.SMEM)
    return pl.pallas_call(
        functools.partial(pool_kernel, copies=copies, tile=tile),
        out_shape=jax.ShapeDtypeStruct((copies, slots, width + META), BF16),
        in_specs=[vmem, smem, smem, any_spec, any_spec, any_spec, vmem],
        out_specs=vmem,
        scratch_shapes=[
            pltpu.VMEM((rows, width), BF16),
            pltpu.VMEM((width, 3 * hidden), BF16),
            pltpu.VMEM((hidden, width), BF16),
            pltpu.VMEM((HEADS, rows, 2 * HEAD_DIM), BF16),
            pltpu.VMEM((HEADS, rows, 2 * HEAD_DIM), BF16),
            pltpu.VMEM((HEADS, HEAD_DIM + ONES, rows), BF16),
            pltpu.VMEM((hidden, tile), BF16),
            pltpu.VMEM((16, width), F32),
            pltpu.SemaphoreType.DMA((8,)),
        ],
        compiler_params=pltpu.CompilerParams(vmem_limit_bytes=POOL_VMEM),
        cost_estimate=pl.CostEstimate(
            flops=2 * rows * width * 4 * hidden + 4 * rows * rows * hidden,
            bytes_accessed=2 * (rows * width + 4 * width * hidden),
            transcendentals=HEADS * rows * rows // 2,
        ),
        name="pool",
    )(seg_ids, counts, positives, tokens, w_qkv, w_out, ln_gain.reshape(1, width))


def gram_kernel(w_hbm, out_ref, w_ref, sems, *, block):
    blocks = out_ref.shape[0] // block
    copies = []
    for b in range(blocks):
        part = slice(b * block, (b + 1) * block)
        copies.append(pltpu.make_async_copy(w_hbm.at[part, :], w_ref.at[part, :], sems.at[b]))
        copies[-1].start()
    for b in range(blocks):
        copies[b].wait()
        right = w_ref[b * block : (b + 1) * block, :]
        for c in range(b + 1):
            left = w_ref[c * block : (c + 1) * block, :]
            value = dot_nt(left, right).astype(BF16)
            out_ref[c * block : (c + 1) * block, b * block : (b + 1) * block] = value
            if c < b:
                out_ref[b * block : (b + 1) * block, c * block : (c + 1) * block] = value.T


def gram_of(w_proj):
    rows, depth = w_proj.shape
    block = 256
    return pl.pallas_call(
        functools.partial(gram_kernel, block=block),
        out_shape=jax.ShapeDtypeStruct((rows, rows), BF16),
        in_specs=[pl.BlockSpec(memory_space=pltpu.HBM)],
        out_specs=pl.BlockSpec(memory_space=pltpu.VMEM),
        scratch_shapes=[
            pltpu.VMEM((rows, depth), BF16),
            pltpu.SemaphoreType.DMA((rows // block,)),
        ],
        compiler_params=pltpu.CompilerParams(vmem_limit_bytes=GRAM_VMEM),
        cost_estimate=pl.CostEstimate(
            flops=2 * rows * rows * depth, bytes_accessed=2 * rows * depth, transcendentals=0
        ),
        name="gram",
    )(w_proj)


def live_spread(meta):
    pick = lax.broadcasted_iota(jnp.int32, (META, 128), 0) == 2
    return dot(meta, pick.astype(F32).astype(BF16))


def column_sums(logit, live, shift):
    rows, columns = logit.shape
    pieces = []
    for c in range(0, columns, 128):
        term = jnp.exp2(logit[:, c : c + 128]) * live
        if shift is not None and shift <= c < shift + rows:
            row = lax.broadcasted_iota(jnp.int32, (rows, 128), 0) + shift
            col = lax.broadcasted_iota(jnp.int32, (rows, 128), 1) + c
            term = jnp.where(row == col, 0.0, term)
        pieces.append(jnp.sum(term.reshape(rows // 8, 8, 128), axis=0))
    return jnp.concatenate(pieces, axis=1)


def own_place(slots):
    z, y, x, _ = (lax.axis_index(a) for a in AXES)
    begin = ((y * 4 + x) * 8 + z) * slots
    return begin, pl.multiple_of(begin // 16 * 16, 16)


def side_kernel(
    pooled_ref,
    gram_ref,
    left_ref,
    right_ref,
    norm_ref,
    line_ref,
    own_logit_ref,
    logit_ref,
    *,
    slots,
    block,
):
    part, width = left_ref.shape
    sides(pooled_ref, gram_ref[...], left_ref, right_ref, norm_ref, 0, block)
    live = live_spread(pooled_ref[:, width:])
    right = right_ref[...]
    sums = jnp.zeros((8, part), F32)
    for b in range(0, part, block):
        rows = slice(b, b + block)
        logit = dot_nt(left_ref[rows, :], right)
        logit_ref[rows, :] = logit
        sums = sums + column_sums(logit, live[rows], b)
    row = lax.broadcasted_iota(jnp.int32, (8, part), 0)
    norms = norm_ref[...].T[0:1]
    sums = jnp.sum(sums, axis=0, keepdims=True)
    line_ref[...] = jnp.where(row == 0, sums, jnp.where(row == 1, norms, 0.0))
    _, base = own_place(slots)
    own_logit_ref[...] = logit_ref[pl.ds(base, 16), :]


def sides(pooled_ref, gram, left_ref, right_ref, norm_ref, place, block):
    width = gram.shape[0]
    for begin in range(0, pooled_ref.shape[0], block):
        rows = slice(place + begin, place + begin + block)
        pooled = pooled_ref[begin : begin + block, 0:width]
        through = dot(pooled, gram)
        wide = pooled.astype(F32)
        square = jnp.sum(through * wide, axis=1, keepdims=True)
        rnorm = lax.rsqrt(jnp.maximum(square, 0.0) + 1e-06)
        left_ref[rows, :] = (through * (rnorm * (LOGIT_SCALE * LOG2E))).astype(BF16)
        right_ref[rows, :] = (wide * rnorm).astype(BF16)
        norm_ref[rows, :] = jnp.broadcast_to(rnorm, (block, norm_ref.shape[1]))


def own_sides(mine, gram, slots):
    part = mine.shape[0]
    width = gram.shape[0]
    vmem = pl.BlockSpec(memory_space=pltpu.VMEM)
    return pl.pallas_call(
        functools.partial(side_kernel, slots=slots, block=256),
        out_shape=(
            jax.ShapeDtypeStruct((part, width), BF16),
            jax.ShapeDtypeStruct((part, width), BF16),
            jax.ShapeDtypeStruct((part, 128), F32),
            jax.ShapeDtypeStruct((8, part), F32),
            jax.ShapeDtypeStruct((16, part), F32),
        ),
        in_specs=[vmem, vmem],
        out_specs=(vmem,) * 5,
        scratch_shapes=[pltpu.VMEM((part, part), F32)],
        compiler_params=pltpu.CompilerParams(vmem_limit_bytes=SIDE_VMEM),
        cost_estimate=pl.CostEstimate(
            flops=2 * part * width * (width + part),
            bytes_accessed=8 * part * width,
            transcendentals=part * part,
        ),
        name="sides",
    )(mine, gram)


def loss_kernel(
    mine_ref,
    other_ref,
    gram_ref,
    own_left_ref,
    own_right_ref,
    own_norm_ref,
    own_line_ref,
    own_logit_ref,
    far_line_ref,
    loss_ref,
    grad_ref,
    logit_ref,
):
    part, width = own_right_ref.shape
    slots = grad_ref.shape[0]
    block = 256

    meta = jnp.concatenate([mine_ref[:, width:], other_ref[:, width:]], axis=0)
    pick = lax.broadcasted_iota(jnp.int32, (16, META), 0) == lax.broadcasted_iota(
        jnp.int32, (16, META), 1
    )
    lines = dot_nt(pick.astype(F32).astype(BF16), meta)
    live = live_spread(mine_ref[:, width:])

    far = other_ref[:, 0:width]
    far_norm = far_line_ref[1:2, :]
    spread_norm = jnp.broadcast_to(far_norm, (block, part))
    far_live = jnp.broadcast_to(lines[2:3, part:], (block, part))
    far_sums = jnp.zeros((8, part), F32)
    row_sums = []
    raws = [dot_nt(own_left_ref[b : b + block, :], far) for b in range(0, part, block)]
    for i, raw in enumerate(raws):
        rows = slice(i * block, (i + 1) * block)
        logit = raw * spread_norm
        logit_ref[rows, :] = logit
        far_sums = far_sums + column_sums(logit, live[rows], None)
        row = jnp.sum(jnp.exp2(logit) * far_live, axis=1, keepdims=True)
        row_sums.append(jnp.broadcast_to(row, (block, 128)))
    own_line = own_line_ref[0:1, :] + jnp.concatenate(row_sums, axis=0).T[0:1]
    far_line = far_line_ref[0:1, :] + jnp.sum(far_sums, axis=0, keepdims=True)
    denominator_line = jnp.concatenate([own_line, far_line], axis=1)

    begin, base = own_place(slots)
    within = begin - base
    own_meta = mine_ref[pl.ds(base, 16), width:].astype(F32)
    own_positive = own_meta[:, 0:1] * 32.0 + own_meta[:, 1:2]
    own_live = own_meta[:, 2:3] > 0.5
    own_slot = own_meta[:, 3:4] * 32.0 + own_meta[:, 4:5]
    positive_line = lines[0:1, :] * 32.0 + lines[1:2, :]
    live_line = lines[2:3, :] > 0.5
    slot_line = lines[3:4, :] * 32.0 + lines[4:5, :]

    logit = jnp.concatenate([own_logit_ref[...], logit_ref[pl.ds(base, 16), :]], axis=1)
    same = slot_line == own_slot
    raw = jnp.where(same, 0.0, jnp.exp2(logit))
    as_query = jnp.where(live_line, raw, 0.0)
    denominator = jnp.sum(as_query, axis=1, keepdims=True)
    target = slot_line == own_positive
    picked = jnp.sum(jnp.where(target, logit, 0.0), axis=1, keepdims=True) * (1.0 / LOG2E)
    loss = jnp.where(own_live, jnp.log(denominator) - picked, 0.0)
    for s in range(slots):
        row = lax.broadcasted_iota(jnp.int32, (16, 1), 0)
        loss_ref[s] = jnp.sum(jnp.where(row == within + s, loss, 0.0))
    query_weights = jnp.where(own_live, as_query / denominator - target.astype(F32), 0.0)
    hits = (positive_line == own_slot).astype(F32)
    key_weights = jnp.where(
        live_line, jnp.where(own_live, raw, 0.0) / denominator_line - hits, 0.0
    )
    weights = query_weights + key_weights
    mix = dot(weights[:, 0:part].astype(BF16), own_right_ref[...])
    mix = mix + dot((weights[:, part:] * far_norm).astype(BF16), far)
    image = dot(mix.astype(BF16), gram_ref[...]) * LOGIT_SCALE
    unit_image = own_left_ref[pl.ds(base, 16), :].astype(F32) * (1.0 / (LOGIT_SCALE * LOG2E))
    radial = LOGIT_SCALE * jnp.sum(mix * unit_image, axis=1, keepdims=True)
    rnorm = own_norm_ref[pl.ds(base, 16), 0:1]
    grad = (image - radial * unit_image) * rnorm
    out = grad[0:slots]
    for i in range(1, 16 // slots):
        out = jnp.where(within == i * slots, grad[i * slots : (i + 1) * slots], out)
    grad_ref[...] = out


def loss_and_grad(mine, other, gram, own, far_line, slots):
    part, padded = mine.shape
    width = padded - META
    vmem = pl.BlockSpec(memory_space=pltpu.VMEM)
    return pl.pallas_call(
        loss_kernel,
        out_shape=(
            jax.ShapeDtypeStruct((slots,), F32),
            jax.ShapeDtypeStruct((slots, width), F32),
        ),
        in_specs=[vmem] * 9,
        out_specs=(pl.BlockSpec(memory_space=pltpu.SMEM), vmem),
        scratch_shapes=[pltpu.VMEM((part, part), F32)],
        compiler_params=pltpu.CompilerParams(vmem_limit_bytes=LOSS_VMEM),
        cost_estimate=pl.CostEstimate(
            flops=2 * part * part * width,
            bytes_accessed=8 * part * width,
            transcendentals=part * part,
        ),
        name="loss",
    )(mine, other, gram, *own, far_line)


def body(tokens, seg_ids, counts, positives, w_qkv, w_out, ln_gain, w_proj):
    slots = positives.shape[0]
    z_size = lax.axis_size("dp_0")
    plane = ("dp_1", "dp_2")
    plane_size = lax.axis_size(plane)
    packed = pooled_rows(tokens, seg_ids, counts, positives, w_qkv, w_out, ln_gain, z_size)
    padded = packed.shape[-1]
    w_proj, packed = lax.optimization_barrier((w_proj, packed))
    gram = gram_of(w_proj)
    line = lax.all_to_all(packed, "dp_0", split_axis=0, concat_axis=0, tiled=True)
    line = line.reshape(z_size * slots, padded)
    line, gram = lax.optimization_barrier((line, gram))
    copies = jnp.broadcast_to(line, (plane_size, *line.shape))
    mine = lax.all_to_all(copies, plane, split_axis=0, concat_axis=0, tiled=True)
    mine = mine.reshape(plane_size * z_size * slots, padded)
    pairs = [(0, 1), (1, 0)]
    other = lax.ppermute(mine, "dp_3", pairs)
    own = own_sides(mine, gram, slots)
    far_line = lax.ppermute(own[3], "dp_3", pairs)
    return loss_and_grad(mine, other, gram, own, far_line, slots)


def solution(mesh):
    finer = Mesh(mesh.devices.reshape(8, 4, 4, 2), AXES)
    return jax.shard_map(
        body,
        mesh=finer,
        in_specs=(P(AXES, None), P(AXES, None), P(), P(AXES), P(), P(), P(), P()),
        out_specs=(P(AXES), P(AXES, None)),
        check_vma=False,
    )
```

```python
import functools
import math

import jax
import jax.numpy as jnp
from jax import lax
from jax.experimental import pallas as pl
from jax.experimental.pallas import tpu as pltpu
from jax.sharding import Mesh
from jax.sharding import PartitionSpec as P

AXES = ("dp_0", "dp_1", "dp_2", "dp_3")
HEADS = 8
HEAD_DIM = 64
PAIRS = HEADS // 2
LOG2E = math.log2(math.e)
LOGIT_SCALE = 20.0
META = 128
ONES = 16
FAR = -1e30
BF16 = jnp.bfloat16
F32 = jnp.float32
POOL_VMEM = 60 * 1024 * 1024
LOSS_VMEM = 24 * 1024 * 1024
GRAM_VMEM = 12 * 1024 * 1024
SIDE_VMEM = 12 * 1024 * 1024


def dot(a, b):
    return lax.dot_general(a, b, (((1,), (0,)), ((), ())), preferred_element_type=F32)


def dot_nt(a, b):
    return lax.dot_general(a, b, (((1,), (1,)), ((), ())), preferred_element_type=F32)


def dot_tn(a, b):
    return lax.dot_general(a, b, (((0,), (0,)), ((), ())), preferred_element_type=F32)


def rank_of():
    z, y, x, core = (lax.axis_index(a) for a in AXES)
    return ((z * 4 + y) * 4 + x) * 2 + core


def pool_kernel(
    seg_ref,
    counts_ref,
    positives_ref,
    x_hbm,
    wqkv_hbm,
    wout_hbm,
    gain_ref,
    out_ref,
    x_ref,
    wqkv_ref,
    wout_ref,
    q_ref,
    k_ref,
    v_ref,
    ctx_ref,
    sums_ref,
    sems,
    *,
    copies,
    tile,
):
    rows, width = x_ref.shape
    slots = out_ref.shape[1]
    hidden = HEADS * HEAD_DIM
    chunk = 512
    chunks = 3 * hidden // chunk

    parts = 2
    x_copies = []
    for r in range(parts):
        some = slice(r * rows // parts, (r + 1) * rows // parts)
        x_copies.append(
            pltpu.make_async_copy(x_hbm.at[some, :], x_ref.at[some, :], sems.at[r])
        )
    w_copies = []
    for c in range(chunks):
        cols = slice(c * chunk, (c + 1) * chunk)
        w_copies.append(
            pltpu.make_async_copy(wqkv_hbm.at[:, cols], wqkv_ref.at[:, cols], sems.at[parts + c])
        )
    wout_copy = pltpu.make_async_copy(wout_hbm, wout_ref, sems.at[parts + chunks])
    for copy in [w_copies[0], *x_copies, *w_copies[1:], wout_copy]:
        copy.start()

    seg = seg_ref[...]
    begins = [jnp.int32(0)]
    for s in range(1, slots):
        begins.append(jnp.sum((seg < s).astype(F32)).astype(jnp.int32))
    begins.append(jnp.int32(rows))

    row_id = lax.broadcasted_iota(jnp.int32, (rows, 2 * HEAD_DIM), 0)
    lane = lax.broadcasted_iota(jnp.int32, (rows, 2 * HEAD_DIM), 1)
    of_row = jnp.zeros((rows, 2 * HEAD_DIM), jnp.int32)
    for s in range(1, slots):
        of_row += (row_id >= begins[s]).astype(jnp.int32)
    feature = lane % HEAD_DIM
    mine = feature == of_row
    q_mark = jnp.where(mine, 1.0, 0.0).astype(BF16)
    k_mark = jnp.where(mine | (feature >= slots), 0.0, FAR).astype(BF16)
    first_half = lane < HEAD_DIM

    def product(kind, some):
        return dot(x_ref[some, :], wqkv_ref[:, kind * hidden : (kind + 1) * hidden])

    def place(kind, some, part):
        if kind == 0:
            part = part * (LOG2E * HEAD_DIM**-0.5)
        part = part.astype(BF16)
        left = first_half[some]
        for p in range(PAIRS):
            pair = part[:, p * 2 * HEAD_DIM : (p + 1) * 2 * HEAD_DIM]
            head = 2 * p
            if kind == 0:
                q_ref[head, some, :] = jnp.where(left, pair, q_mark[some])
                q_ref[head + 1, some, :] = jnp.where(left, q_mark[some], pair)
            elif kind == 1:
                k_ref[head, some, :] = jnp.where(left, pair, k_mark[some])
                k_ref[head + 1, some, :] = jnp.where(left, k_mark[some], pair)
            else:
                turned = pair.T
                for i in range(2):
                    v_ref[head + i, 0:HEAD_DIM, some] = turned[i * HEAD_DIM : (i + 1) * HEAD_DIM]
                    v_ref[head + i, HEAD_DIM:, some] = jnp.ones((ONES, turned.shape[1]), BF16)

    def in_turn(steps):
        ahead = product(*steps[0])
        for i, step in enumerate(steps):
            part = ahead
            if i + 1 < len(steps):
                ahead = product(*steps[i + 1])
            place(*step, part)

    pieces = [slice(r * rows // parts, (r + 1) * rows // parts) for r in range(parts)]
    w_copies[0].wait()
    for r in range(parts):
        x_copies[r].wait()
        in_turn([(0, pieces[r])])
    w_copies[1].wait()
    w_copies[2].wait()
    in_turn([(kind, some) for kind in (1, 2) for some in pieces])

    wout_copy.wait()
    sums_ref[...] = jnp.zeros_like(sums_ref)
    ctx_ref[...] = jnp.zeros_like(ctx_ref)
    key_tile = 128
    key_tiles = rows // key_tile
    widths = [w for w in (3, 4, 5, 6, 8) if w <= key_tiles]

    def project_out(r0):
        return x_ref[pl.ds(r0, tile), :].astype(F32) + dot_tn(ctx_ref[...], wout_ref[...])

    def pool_tile(resid, r0, valid):
        centre = resid - jnp.mean(resid, axis=1, keepdims=True)
        variance = jnp.mean(centre * centre, axis=1, keepdims=True)
        out = (centre * lax.rsqrt(variance + 1e-05) * gain_ref[...]).astype(BF16)
        slot = lax.broadcasted_iota(jnp.int32, (16, tile), 0)
        token = lax.broadcasted_iota(jnp.int32, (16, tile), 1) + r0
        member = jnp.zeros((16, tile), jnp.bool_)
        for s in range(slots):
            member |= (slot == s) & (token >= begins[s]) & (token < begins[s + 1])
        member = jnp.where(member & valid, 1.0, 0.0).astype(BF16)
        sums_ref[...] += dot(member, out)

    def one_tile(t, carry):
        r0 = pl.multiple_of(t * tile, tile)
        last = pl.multiple_of(jnp.maximum(r0 - tile, 0), tile)
        low = jnp.int32(0)
        high = jnp.int32(rows)
        for s in range(1, slots):
            low = jnp.where(begins[s] <= r0, begins[s], low)
        for s in range(slots - 1, 0, -1):
            high = jnp.where(begins[s] >= r0 + tile, begins[s], high)
        k0 = low // key_tile
        need = (high + key_tile - 1) // key_tile - k0

        for i, w in enumerate(widths):
            above = widths[i - 1] if i else 0

            @pl.when((need > above) & (need <= w))
            def _():
                start = pl.multiple_of(jnp.minimum(k0, key_tiles - w) * key_tile, key_tile)
                def score(h):
                    q = q_ref[h, pl.ds(r0, tile), :]
                    k = k_ref[h, pl.ds(start, w * key_tile), :]
                    return dot_nt(k, q)

                def soften(s):
                    return jnp.exp2(s - jnp.max(s, axis=0, keepdims=True)).astype(BF16)

                def finish(h, e):
                    v = v_ref[h, :, pl.ds(start, w * key_tile)]
                    out = dot(v, e)
                    part = out[0:HEAD_DIM] / out[HEAD_DIM : HEAD_DIM + 1]
                    ctx_ref[h * HEAD_DIM : (h + 1) * HEAD_DIM, :] = part.astype(BF16)

                resid = project_out(last)
                scores = [score(h) for h in range(4)]
                soft = []
                for h in range(HEADS):
                    if h + 4 < HEADS:
                        scores.append(score(h + 4))
                    soft.append(soften(scores[h]))
                    if h >= 2:
                        finish(h - 2, soft[h - 2])
                    if h == 2:
                        pool_tile(resid, last, t > 0)
                for h in range(HEADS - 2, HEADS):
                    finish(h, soft[h])

        return carry

    lax.fori_loop(0, rows // tile, one_tile, 0)
    last = rows - tile
    pool_tile(project_out(last), last, True)

    slot_col = lax.broadcasted_iota(jnp.int32, (slots, 1), 0)
    sizes = jnp.ones((slots, 1), F32)
    for s in range(slots):
        sizes = jnp.where(slot_col == s, (begins[s + 1] - begins[s]).astype(F32), sizes)
    pooled = (sums_ref[0:slots, :] / sizes).astype(BF16)

    rank = rank_of()
    count = counts_ref[rank]
    line = lax.broadcasted_iota(jnp.int32, (slots, META), 0)
    col = lax.broadcasted_iota(jnp.int32, (slots, META), 1)
    positive = jnp.zeros((slots, META), jnp.int32)
    for s in range(slots):
        positive = jnp.where(line == s, positives_ref[s], positive)
    own = rank * slots + line
    meta = jnp.where(col == 0, positive >> 5, 0)
    meta = jnp.where(col == 1, positive & 31, meta)
    meta = jnp.where(col == 2, (line < count).astype(jnp.int32), meta)
    meta = jnp.where(col == 3, own >> 5, meta)
    meta = jnp.where(col == 4, own & 31, meta)
    meta = meta.astype(F32).astype(BF16)
    for i in range(copies):
        out_ref[i, :, 0:width] = pooled
        out_ref[i, :, width:] = meta


def pooled_rows(tokens, seg_ids, counts, positives, w_qkv, w_out, ln_gain, copies):
    rows, width = tokens.shape
    slots = positives.shape[0]
    hidden = w_out.shape[0]
    tile = 256
    any_spec = pl.BlockSpec(memory_space=pltpu.HBM)
    vmem = pl.BlockSpec(memory_space=pltpu.VMEM)
    smem = pl.BlockSpec(memory_space=pltpu.SMEM)
    return pl.pallas_call(
        functools.partial(pool_kernel, copies=copies, tile=tile),
        out_shape=jax.ShapeDtypeStruct((copies, slots, width + META), BF16),
        in_specs=[vmem, smem, smem, any_spec, any_spec, any_spec, vmem],
        out_specs=vmem,
        scratch_shapes=[
            pltpu.VMEM((rows, width), BF16),
            pltpu.VMEM((width, 3 * hidden), BF16),
            pltpu.VMEM((hidden, width), BF16),
            pltpu.VMEM((HEADS, rows, 2 * HEAD_DIM), BF16),
            pltpu.VMEM((HEADS, rows, 2 * HEAD_DIM), BF16),
            pltpu.VMEM((HEADS, HEAD_DIM + ONES, rows), BF16),
            pltpu.VMEM((hidden, tile), BF16),
            pltpu.VMEM((16, width), F32),
            pltpu.SemaphoreType.DMA((8,)),
        ],
        compiler_params=pltpu.CompilerParams(vmem_limit_bytes=POOL_VMEM),
        cost_estimate=pl.CostEstimate(
            flops=2 * rows * width * 4 * hidden + 4 * rows * rows * hidden,
            bytes_accessed=2 * (rows * width + 4 * width * hidden),
            transcendentals=HEADS * rows * rows // 2,
        ),
        name="pool",
    )(seg_ids, counts, positives, tokens, w_qkv, w_out, ln_gain.reshape(1, width))


def gram_kernel(w_ref, out_ref, *, block):
    for b in range(out_ref.shape[0] // block):
        right = w_ref[b * block : (b + 1) * block, :]
        for c in range(b + 1):
            left = w_ref[c * block : (c + 1) * block, :]
            value = dot_nt(left, right).astype(BF16)
            out_ref[c * block : (c + 1) * block, b * block : (b + 1) * block] = value
            if c < b:
                out_ref[b * block : (b + 1) * block, c * block : (c + 1) * block] = value.T


def gram_of(w_proj):
    rows, depth = w_proj.shape
    vmem = pl.BlockSpec(memory_space=pltpu.VMEM)
    return pl.pallas_call(
        functools.partial(gram_kernel, block=256),
        out_shape=jax.ShapeDtypeStruct((rows, rows), BF16),
        in_specs=[vmem],
        out_specs=vmem,
        compiler_params=pltpu.CompilerParams(vmem_limit_bytes=GRAM_VMEM),
        cost_estimate=pl.CostEstimate(
            flops=2 * rows * rows * depth, bytes_accessed=2 * rows * depth, transcendentals=0
        ),
        name="gram",
    )(w_proj)


def live_spread(meta):
    pick = lax.broadcasted_iota(jnp.int32, (META, 128), 0) == 2
    return dot(meta, pick.astype(F32).astype(BF16))


def column_sums(logit, live, shift):
    rows, columns = logit.shape
    pieces = []
    for c in range(0, columns, 128):
        term = jnp.exp2(logit[:, c : c + 128]) * live
        if shift is not None and shift <= c < shift + rows:
            row = lax.broadcasted_iota(jnp.int32, (rows, 128), 0) + shift
            col = lax.broadcasted_iota(jnp.int32, (rows, 128), 1) + c
            term = jnp.where(row == col, 0.0, term)
        pieces.append(jnp.sum(term.reshape(rows // 8, 8, 128), axis=0))
    return jnp.concatenate(pieces, axis=1)


def own_place(slots):
    z, y, x, _ = (lax.axis_index(a) for a in AXES)
    begin = ((y * 4 + x) * 8 + z) * slots
    return begin, pl.multiple_of(begin // 16 * 16, 16)


def side_kernel(
    pooled_ref,
    gram_ref,
    left_ref,
    right_ref,
    norm_ref,
    line_ref,
    own_logit_ref,
    logit_ref,
    *,
    slots,
    block,
):
    part, width = left_ref.shape
    sides(pooled_ref, gram_ref[...], left_ref, right_ref, norm_ref, 0, block)
    live = live_spread(pooled_ref[:, width:])
    right = right_ref[...]
    sums = jnp.zeros((8, part), F32)
    for b in range(0, part, block):
        rows = slice(b, b + block)
        logit = dot_nt(left_ref[rows, :], right)
        logit_ref[rows, :] = logit
        sums = sums + column_sums(logit, live[rows], b)
    row = lax.broadcasted_iota(jnp.int32, (8, part), 0)
    norms = norm_ref[...].T[0:1]
    sums = jnp.sum(sums, axis=0, keepdims=True)
    line_ref[...] = jnp.where(row == 0, sums, jnp.where(row == 1, norms, 0.0))
    _, base = own_place(slots)
    own_logit_ref[...] = logit_ref[pl.ds(base, 16), :]


def sides(pooled_ref, gram, left_ref, right_ref, norm_ref, place, block):
    width = gram.shape[0]
    for begin in range(0, pooled_ref.shape[0], block):
        rows = slice(place + begin, place + begin + block)
        pooled = pooled_ref[begin : begin + block, 0:width]
        through = dot(pooled, gram)
        wide = pooled.astype(F32)
        square = jnp.sum(through * wide, axis=1, keepdims=True)
        rnorm = lax.rsqrt(jnp.maximum(square, 0.0) + 1e-06)
        left_ref[rows, :] = (through * (rnorm * (LOGIT_SCALE * LOG2E))).astype(BF16)
        right_ref[rows, :] = (wide * rnorm).astype(BF16)
        norm_ref[rows, :] = jnp.broadcast_to(rnorm, (block, norm_ref.shape[1]))


def own_sides(mine, gram, slots):
    part = mine.shape[0]
    width = gram.shape[0]
    vmem = pl.BlockSpec(memory_space=pltpu.VMEM)
    return pl.pallas_call(
        functools.partial(side_kernel, slots=slots, block=256),
        out_shape=(
            jax.ShapeDtypeStruct((part, width), BF16),
            jax.ShapeDtypeStruct((part, width), BF16),
            jax.ShapeDtypeStruct((part, 128), F32),
            jax.ShapeDtypeStruct((8, part), F32),
            jax.ShapeDtypeStruct((16, part), F32),
        ),
        in_specs=[vmem, vmem],
        out_specs=(vmem,) * 5,
        scratch_shapes=[pltpu.VMEM((part, part), F32)],
        compiler_params=pltpu.CompilerParams(vmem_limit_bytes=SIDE_VMEM),
        cost_estimate=pl.CostEstimate(
            flops=2 * part * width * (width + part),
            bytes_accessed=8 * part * width,
            transcendentals=part * part,
        ),
        name="sides",
    )(mine, gram)


def cross_kernel(left_ref, other_ref, raw_ref, *, block):
    part, width = left_ref.shape
    far = other_ref[:, 0:width]
    for b in range(0, part, block):
        raw_ref[b : b + block, :] = dot_nt(left_ref[b : b + block, :], far)


def cross_logits(left, other):
    part, width = left.shape
    vmem = pl.BlockSpec(memory_space=pltpu.VMEM)
    return pl.pallas_call(
        functools.partial(cross_kernel, block=256),
        out_shape=jax.ShapeDtypeStruct((part, part), F32),
        in_specs=[vmem, vmem],
        out_specs=vmem,
        compiler_params=pltpu.CompilerParams(vmem_limit_bytes=SIDE_VMEM),
        cost_estimate=pl.CostEstimate(
            flops=2 * part * part * width, bytes_accessed=8 * part * width, transcendentals=0
        ),
        name="cross",
    )(left, other)


def loss_kernel(
    mine_ref,
    other_ref,
    gram_ref,
    own_left_ref,
    own_right_ref,
    own_norm_ref,
    own_line_ref,
    own_logit_ref,
    far_line_ref,
    raw_ref,
    loss_ref,
    grad_ref,
    logit_ref,
):
    part, width = own_right_ref.shape
    slots = grad_ref.shape[0]
    block = 256

    meta = jnp.concatenate([mine_ref[:, width:], other_ref[:, width:]], axis=0)
    pick = lax.broadcasted_iota(jnp.int32, (16, META), 0) == lax.broadcasted_iota(
        jnp.int32, (16, META), 1
    )
    lines = dot_nt(pick.astype(F32).astype(BF16), meta)
    live = live_spread(mine_ref[:, width:])

    far = other_ref[:, 0:width]
    far_norm = far_line_ref[1:2, :]
    spread_norm = jnp.broadcast_to(far_norm, (block, part))
    far_live = jnp.broadcast_to(lines[2:3, part:], (block, part))
    far_sums = jnp.zeros((8, part), F32)
    row_sums = []
    raws = [raw_ref[b : b + block, :] for b in range(0, part, block)]
    for i, raw in enumerate(raws):
        rows = slice(i * block, (i + 1) * block)
        logit = raw * spread_norm
        logit_ref[rows, :] = logit
        far_sums = far_sums + column_sums(logit, live[rows], None)
        row = jnp.sum(jnp.exp2(logit) * far_live, axis=1, keepdims=True)
        row_sums.append(jnp.broadcast_to(row, (block, 128)))
    own_line = own_line_ref[0:1, :] + jnp.concatenate(row_sums, axis=0).T[0:1]
    far_line = far_line_ref[0:1, :] + jnp.sum(far_sums, axis=0, keepdims=True)
    denominator_line = jnp.concatenate([own_line, far_line], axis=1)

    begin, base = own_place(slots)
    within = begin - base
    own_meta = mine_ref[pl.ds(base, 16), width:].astype(F32)
    own_positive = own_meta[:, 0:1] * 32.0 + own_meta[:, 1:2]
    own_live = own_meta[:, 2:3] > 0.5
    own_slot = own_meta[:, 3:4] * 32.0 + own_meta[:, 4:5]
    positive_line = lines[0:1, :] * 32.0 + lines[1:2, :]
    live_line = lines[2:3, :] > 0.5
    slot_line = lines[3:4, :] * 32.0 + lines[4:5, :]

    logit = jnp.concatenate([own_logit_ref[...], logit_ref[pl.ds(base, 16), :]], axis=1)
    same = slot_line == own_slot
    raw = jnp.where(same, 0.0, jnp.exp2(logit))
    as_query = jnp.where(live_line, raw, 0.0)
    denominator = jnp.sum(as_query, axis=1, keepdims=True)
    target = slot_line == own_positive
    picked = jnp.sum(jnp.where(target, logit, 0.0), axis=1, keepdims=True) * (1.0 / LOG2E)
    loss = jnp.where(own_live, jnp.log(denominator) - picked, 0.0)
    for s in range(slots):
        row = lax.broadcasted_iota(jnp.int32, (16, 1), 0)
        loss_ref[s] = jnp.sum(jnp.where(row == within + s, loss, 0.0))
    query_weights = jnp.where(own_live, as_query / denominator - target.astype(F32), 0.0)
    hits = (positive_line == own_slot).astype(F32)
    key_weights = jnp.where(
        live_line, jnp.where(own_live, raw, 0.0) / denominator_line - hits, 0.0
    )
    weights = query_weights + key_weights
    mix = dot(weights[:, 0:part].astype(BF16), own_right_ref[...])
    mix = mix + dot((weights[:, part:] * far_norm).astype(BF16), far)
    image = dot(mix.astype(BF16), gram_ref[...]) * LOGIT_SCALE
    unit_image = own_left_ref[pl.ds(base, 16), :].astype(F32) * (1.0 / (LOGIT_SCALE * LOG2E))
    radial = LOGIT_SCALE * jnp.sum(mix * unit_image, axis=1, keepdims=True)
    rnorm = own_norm_ref[pl.ds(base, 16), 0:1]
    grad = (image - radial * unit_image) * rnorm
    out = grad[0:slots]
    for i in range(1, 16 // slots):
        out = jnp.where(within == i * slots, grad[i * slots : (i + 1) * slots], out)
    grad_ref[...] = out


def loss_and_grad(mine, other, gram, own, far_line, raw, slots):
    part, padded = mine.shape
    width = padded - META
    vmem = pl.BlockSpec(memory_space=pltpu.VMEM)
    return pl.pallas_call(
        loss_kernel,
        out_shape=(
            jax.ShapeDtypeStruct((slots,), F32),
            jax.ShapeDtypeStruct((slots, width), F32),
        ),
        in_specs=[vmem] * 10,
        out_specs=(pl.BlockSpec(memory_space=pltpu.SMEM), vmem),
        scratch_shapes=[pltpu.VMEM((part, part), F32)],
        compiler_params=pltpu.CompilerParams(vmem_limit_bytes=LOSS_VMEM),
        cost_estimate=pl.CostEstimate(
            flops=2 * part * part * width,
            bytes_accessed=8 * part * width,
            transcendentals=part * part,
        ),
        name="loss",
    )(mine, other, gram, *own, far_line, raw)


def body(tokens, seg_ids, counts, positives, w_qkv, w_out, ln_gain, w_proj):
    slots = positives.shape[0]
    z_size = lax.axis_size("dp_0")
    plane = ("dp_1", "dp_2")
    plane_size = lax.axis_size(plane)
    packed = pooled_rows(tokens, seg_ids, counts, positives, w_qkv, w_out, ln_gain, z_size)
    padded = packed.shape[-1]
    w_proj, packed = lax.optimization_barrier((w_proj, packed))
    gram = gram_of(w_proj)
    line = lax.all_to_all(packed, "dp_0", split_axis=0, concat_axis=0, tiled=True)
    line = line.reshape(z_size * slots, padded)
    line, gram = lax.optimization_barrier((line, gram))
    copies = jnp.broadcast_to(line, (plane_size, *line.shape))
    mine = lax.all_to_all(copies, plane, split_axis=0, concat_axis=0, tiled=True)
    mine = mine.reshape(plane_size * z_size * slots, padded)
    pairs = [(0, 1), (1, 0)]
    other = lax.ppermute(mine, "dp_3", pairs)
    own = own_sides(mine, gram, slots)
    far_line = lax.ppermute(own[3], "dp_3", pairs)
    raw = cross_logits(own[0], other)
    return loss_and_grad(mine, other, gram, own, far_line, raw, slots)


def solution(mesh):
    finer = Mesh(mesh.devices.reshape(8, 4, 4, 2), AXES)
    return jax.shard_map(
        body,
        mesh=finer,
        in_specs=(P(AXES, None), P(AXES, None), P(), P(AXES), P(), P(), P(), P()),
        out_specs=(P(AXES), P(AXES, None)),
        check_vma=False,
    )
```
